256 devices in a mesh: seq: 4 (over y), tp: 8 (over z), grp: 8 (over x, core).
Axes of the slice: x: 4, y: 4, z: 8, core: 2. Of those that a mesh axis runs over, the one named last changes fastest.
Arguments:
- queries: bfloat16 [16, 64, 128], P('grp', 'tp'), may hold values from -2000 to 2000
- cache_pool: bfloat16 [2048, 8, 2, 128, 128], P(('seq', 'grp'), 'tp'), may hold values from -6 to 6
- block_scale: bfloat16 [2048, 8, 2], P(('seq', 'grp'), 'tp'), may hold values from 0.29 to 3
- block_table: int32 [16, 128], replicated, may hold values from 0 to 2047, as said below
- lengths: int32 [16], replicated, may hold values from 128 to 16384
- output_weight: bfloat16 [8192, 8192], P('tp', ('seq', 'grp')), may hold values from -0.0625 to 0.0625
Outputs:
- attention_output: bfloat16 [16, 8192], P('tp', ('seq', 'grp'))
- decode_cache: bfloat16 [16, 128, 8, 2, 128, 128], P('grp', 'seq', 'tp')
- decode_scale: bfloat16 [16, 128, 8, 2], P('grp', 'seq', 'tp')
The draws below stay inside these ranges and needn't reach their ends.
Inputs may be any that keep to these rules, and one draw needn't show every extreme that they name: block_table names every pool slot exactly once. Take any run of 64 slots starting at a multiple of 64, any group of 2 consecutive requests starting at a multiple of 2, and any range of 32 block positions starting at a multiple of 32: exactly 2 slots of the run hold blocks of those requests at those positions.
All inputs are finite; a program needn't handle non-finite values.
Results may differ from the reference program's by a relative error of at most 0.014.
Values may be sent and summed in bfloat16 or wider, within the bound.
No kernel may reach another device: no remote copies, remote signals or barrier semaphores. Data moves between devices by JAX's collectives and lax.ppermute only.
A program may use at most 64 MiB of HBM per device.

```python
import math
import jax
import jax.numpy as jnp
from jax import lax

D = 8192
H = 64
KVH = 8
HD = 128
BLK = 128
NB = 128
BPG = 2
BATCH = 16
POOL = 2048
POOL_DEV = 64
NBQ = 32
CAP = 2
N_SEQ = 4
N_GRP = 8


def block_layout(key):
    base_key = jax.random.fold_in(key, 7)
    pair_keys = jax.random.split(jax.random.fold_in(base_key, 1), N_GRP * N_SEQ)
    spread = jax.vmap(lambda sub_key: jax.random.permutation(sub_key, BPG * NBQ))(pair_keys).astype(jnp.int32)
    owner_keys = jax.random.split(jax.random.fold_in(base_key, 2), N_SEQ * N_GRP)
    places = jax.vmap(lambda sub_key: jax.random.permutation(sub_key, POOL_DEV))(owner_keys).astype(jnp.int32)
    owners = spread // CAP
    within = spread % CAP
    pair_ids = jnp.arange(N_GRP * N_SEQ, dtype=jnp.int32)[:, None]
    column = pair_ids * CAP + within
    slot_ids = owners * POOL_DEV + places[owners, column]
    return slot_ids.reshape(N_GRP, N_SEQ, BPG, NBQ).transpose(0, 2, 1, 3).reshape(BATCH, NB).astype(jnp.int32)


def cache_law(key):
    base_key = jax.random.fold_in(key, 13)
    pool_shape = (POOL, KVH, 2, BLK, HD)
    pool_data = jnp.clip(jax.random.normal(jax.random.fold_in(base_key, 1), pool_shape, jnp.float32), -6.0, 6.0)
    scale_data = jnp.exp(jax.random.uniform(jax.random.fold_in(base_key, 2), (POOL, KVH, 2), jnp.float32, math.log(0.5), math.log(2.0)))
    query_data = jnp.clip(2.5 * jax.random.normal(jax.random.fold_in(base_key, 3), (BATCH, H, HD), jnp.float32), -15.0, 15.0)
    return (pool_data, scale_data, query_data)


def draw_queries(key, part):
    return cache_law(key)[2].astype(jnp.bfloat16)


def draw_cache_pool(key, part):
    return cache_law(key)[0].astype(jnp.bfloat16)


def draw_block_scale(key, part):
    return cache_law(key)[1].astype(jnp.bfloat16)


def draw_block_table(key, part):
    return block_layout(key)


def set_ends(drawn, rng, smallest, high):
    spot = [jax.random.randint(jax.random.fold_in(rng, axis), (), 0, length) for axis, length in enumerate(drawn.shape)]
    widest = drawn.shape.index(max(drawn.shape))
    beside = spot[:widest] + [(spot[widest] + 1) % drawn.shape[widest]] + spot[widest + 1:]
    return drawn.at[tuple(spot)].set(smallest).at[tuple(beside)].set(high)


def level_of(own_key, shape, cuts, least, largest):
    def one(position, blocks):
        steps = jax.random.uniform(jax.random.fold_in(jax.random.fold_in(own_key, 6), position), (blocks,), jnp.float32, least / len(cuts), largest / len(cuts))
        return jnp.repeat(jnp.exp(steps), shape[position] // blocks).reshape((-1,) + (1,) * (len(shape) - position - 1))

    factor_of = one(*cuts[0])
    for cut in cuts[1:]:
        factor_of = factor_of * one(*cut)
    return factor_of


def gaussian(rng, extent, deviation, most, cuts=(), held_as=jnp.bfloat16):
    array = deviation * jax.random.normal(rng, extent, jnp.float32)
    if cuts:
        array = array * level_of(rng, extent, cuts, -0.22, 0.18)
    return jnp.clip(array, -most, most).astype(held_as)


def setup_inputs(seed: int = 0) -> dict:
    key_list = jax.random.split(jax.random.key(seed), 7)
    return {
        "queries": draw_queries(jax.random.fold_in(key_list[6], 71), 0),
        "cache_pool": draw_cache_pool(jax.random.fold_in(key_list[6], 71), 0),
        "block_scale": draw_block_scale(jax.random.fold_in(key_list[6], 71), 0),
        "block_table": draw_block_table(jax.random.fold_in(key_list[6], 71), 0),
        "lengths": set_ends(jax.random.randint(key_list[4], (BATCH,), BLK, NB * BLK + 1), jax.random.fold_in(key_list[4], 1), BLK, NB * BLK).astype(jnp.int32),
        "output_weight": gaussian(key_list[5], (H * HD, D), (H * HD) ** -0.5, 0.0625, ((0, 8), (1, 32))),
    }


def reference(queries, cache_pool, block_scale, block_table, lengths, output_weight):
    decode_cache = cache_pool[block_table]
    decode_scale = block_scale[block_table]
    groups = H // KVH
    root_scale = 1.0 / math.sqrt(HD)
    offsets = jnp.arange(NB * BLK, dtype=jnp.int32).reshape(NB, BLK)

    def one_request(request_items):
        query_rows, blocks, scales, length = request_items
        key_rows = blocks[:, :, 0].astype(jnp.float32)
        value_rows = blocks[:, :, 1].astype(jnp.float32)
        head_rows = query_rows.reshape(KVH, groups, HD).astype(jnp.float32)
        scores = jnp.einsum('kgd,nktd->nkgt', head_rows, key_rows, precision=lax.Precision.HIGHEST)
        scores = scores * scales[:, :, 0].astype(jnp.float32)[:, :, None, None] * root_scale
        live_mask = (offsets < length)[:, None, None, :]
        scores = jnp.where(live_mask, scores, -jnp.inf)
        peak = lax.optimization_barrier(jnp.max(scores, axis=(0, 3)))
        weight = jnp.where(live_mask, jnp.exp(scores - peak[None, :, :, None]), 0.0)
        denominator = lax.optimization_barrier(jnp.sum(weight, axis=(0, 3)))
        scaled = (weight * scales[:, :, 1].astype(jnp.float32)[:, :, None, None]).astype(jnp.bfloat16)
        numerator = jnp.einsum('nkgt,nktd->kgd', scaled.astype(jnp.float32), value_rows, precision=lax.Precision.HIGHEST)
        return (numerator / denominator[:, :, None]).astype(jnp.bfloat16).reshape(H * HD)
    attended = lax.map(one_request, (queries, decode_cache, decode_scale, lengths))
    attention_output = jnp.dot(attended, output_weight, preferred_element_type=jnp.float32).astype(jnp.bfloat16)
    return (attention_output, decode_cache, decode_scale)
```

```python
import functools
import math

import jax
import jax.numpy as jnp
from jax import lax
from jax.experimental import pallas as pl
from jax.experimental.pallas import tpu as pltpu
from jax.sharding import PartitionSpec as P

absent_score = -1e30
both_axes = ("seq", "grp")
far = 1 << 20
scale_rows = 8


def sent_to_all(array, axis):
    length = lax.axis_size(axis)
    return lax.all_to_all(
        jnp.broadcast_to(array[None], (length, *array.shape)), axis, 0, 0, tiled=True
    )


def gathered_once(array, axis):
    leaves = jax.tree.leaves(array)
    sequence = sorted(range(len(leaves)), key=lambda k: -leaves[k].size)
    width = (1, *leaves[sequence[0]].shape)[-1]
    lines = [
        jnp.pad(leaves[k].reshape(-1), (0, -leaves[k].size % width)).reshape(-1, width)
        for k in sequence
    ]
    both, at, found = (sent_to_all(jnp.concatenate(lines), axis), 0, {})
    for k, line in zip(sequence, lines):
        share = both[:, at : at + len(line)].reshape(len(both), -1)
        found[k] = share[:, : leaves[k].size].reshape(-1, *leaves[k].shape)
        at += len(line)
    numbers = iter(range(len(leaves)))
    return jax.tree.map(lambda _: found[next(numbers)], array)


def joined_by_halves(pieces, combine):
    while len(jax.tree.leaves(pieces)[0]) > 1:
        pieces = jax.vmap(combine)(
            *(jax.tree.map(lambda part: part[side::2], pieces) for side in (0, 1))
        )
    return jax.tree.map(lambda part: part[0], pieces)


def joined_all(array, axis, combine):
    pieces = gathered_once(array, axis)
    return joined_by_halves(pieces, combine)


def in_order(pieces, dim):
    pieces = jnp.moveaxis(pieces, 0, dim)
    dims = pieces.shape
    return pieces.reshape(*dims[:dim], dims[dim] * dims[dim + 1], *dims[dim + 2 :])


def gather_directly(array, axis, dim):
    pieces = sent_to_all(array, axis)
    return in_order(pieces, dim)


def in_blocks(array, dim, length):
    dims = array.shape
    pieces = array.reshape(*dims[:dim], length, dims[dim] // length, *dims[dim + 1 :])
    return jnp.moveaxis(pieces, dim, 0)


def sum_at_owner(array, axis, dim):
    pieces = in_blocks(array, dim, lax.axis_size(axis))
    arrived = lax.all_to_all(pieces, axis, split_axis=0, concat_axis=0, tiled=True)
    return arrived.sum(axis=0)


def block_scores(block_queries, key_rows, key_scale, live_mask, root_scale):
    scores = jnp.einsum(
        "nkgd,nktd->nkgt", block_queries, key_rows, preferred_element_type=jnp.float32
    )
    scores = scores * key_scale[:, :, None, None] * root_scale
    return jnp.where(live_mask[:, None, None, :], scores, absent_score)


def block_terms(scores, peak_rows, live_mask, value_rows, value_scale):
    weight = jnp.where(live_mask[:, None, None, :], jnp.exp(scores - peak_rows[..., None]), 0.0)
    weight_sum = jnp.sum(weight, axis=-1)
    scaled = (weight * value_scale[:, :, None, None]).astype(jnp.bfloat16)
    partial_sum = jnp.einsum(
        "nkgt,nktd->nkgd", scaled, value_rows, preferred_element_type=jnp.float32
    )
    return (weight_sum, partial_sum)


def combine(former, latter):
    peak_former, sum_former, accum_former = former
    peak_latter, sum_latter, accum_latter = latter
    peak_both = jnp.maximum(peak_former, peak_latter)
    factor_former = jnp.exp(peak_former - peak_both)
    factor_latter = jnp.exp(peak_latter - peak_both)
    return (
        peak_both,
        sum_former * factor_former + sum_latter * factor_latter,
        accum_former * factor_former[..., None] + accum_latter * factor_latter[..., None],
    )


def outgoing_codes(block_table, source, slots, groups, ranges):
    rows, width = block_table.shape
    per_group, span = rows // groups, width // ranges
    table = block_table.reshape(groups, per_group, width)
    column = lax.broadcasted_iota(jnp.int32, table.shape, 2)
    row = lax.broadcasted_iota(jnp.int32, table.shape, 1)
    code = (row * span + column % span) * slots + table % slots
    mine = (table // slots == source)[:, :, None, :] & (
        (column // span)[:, :, None, :] == jnp.arange(ranges, dtype=jnp.int32)[None, None, :, None]
    )
    code = jnp.broadcast_to(code[:, :, None, :], mine.shape)
    return (
        jnp.min(jnp.where(mine, code, far), axis=(1, 3)),
        jnp.max(jnp.where(mine, code, -1), axis=(1, 3)),
    )


def arrival_places(block_table, seq_index, group_index, slots, groups, ranges):
    rows, width = block_table.shape
    per_group, span = rows // groups, width // ranges
    own = lax.dynamic_slice(
        block_table, (group_index * per_group, seq_index * span), (per_group, span)
    )
    source = (own // slots)[None]
    place = lax.broadcasted_iota(jnp.int32, (1, per_group, span), 1) * span
    place = place + lax.broadcasted_iota(jnp.int32, (1, per_group, span), 2)
    here = source == jnp.arange(groups * ranges, dtype=jnp.int32)[:, None, None]
    return (
        jnp.min(jnp.where(here, place, far), axis=(1, 2)),
        jnp.max(jnp.where(here, place, -1), axis=(1, 2)),
    )


def gather_kernel(groups, ranges, slots, first, second, scales, pool, out, held, in_sem, out_sem):
    rows = pool.shape[1]
    copies = []
    for s in range(ranges):
        for g in range(groups):
            d = s * groups + g
            for k, codes in enumerate((first, second)):
                slot = lax.rem(codes[g, s], slots)
                copy = pltpu.make_async_copy(
                    pool.at[slot], held.at[d, pl.ds(k * rows, rows)], in_sem.at[2 * d + k]
                )
                copy.start()
                copies.append(copy)
    row = lax.broadcasted_iota(jnp.int32, (scale_rows, 128), 0)
    lane = lax.broadcasted_iota(jnp.int32, (scale_rows, 128), 1)
    for s in range(ranges):
        for g in range(groups):
            d = s * groups + g
            one, two = (lax.rem(codes[g, s], slots) for codes in (first, second))
            keys = jnp.where(row == 0, scales[2 * one], scales[2 * two])
            values = jnp.where(row == 0, scales[2 * one + 1], scales[2 * two + 1])
            held[d, pl.ds(2 * rows, scale_rows)] = jnp.where(lane == 0, keys, values).astype(
                held.dtype
            )
    sent = []
    for d in range(groups * ranges):
        for k in range(2):
            copies[2 * d + k].wait()
        copy = pltpu.make_async_copy(held.at[d], out.at[d], out_sem.at[d])
        copy.start()
        sent.append(copy)
    for copy in sent:
        copy.wait()


def place_kernel(first, second, arrived, cache, scale, held, in_sem, out_sem):
    sources = arrived.shape[0]
    rows = cache.shape[1]
    copies = []
    for d in range(sources):
        copy = pltpu.make_async_copy(arrived.at[d], held.at[d], in_sem.at[d])
        copy.start()
        copies.append(copy)
    sent = []
    for d in range(sources):
        copies[d].wait()
        for k, places in enumerate((first, second)):
            copy = pltpu.make_async_copy(
                held.at[d, pl.ds(k * rows, rows)], cache.at[places[d]], out_sem.at[2 * d + k]
            )
            copy.start()
            sent.append(copy)
        tile = held[d, pl.ds(2 * rows, scale_rows)].astype(jnp.float32)
        for k, places in enumerate((first, second)):
            scale[pl.ds(places[d], 1), :] = tile[k : k + 1]
    for copy in sent:
        copy.wait()


smem = pl.BlockSpec(memory_space=pltpu.SMEM)
vmem = pl.BlockSpec(memory_space=pltpu.VMEM)
anywhere = pl.BlockSpec(memory_space=pl.ANY)
small_grant = 16 * 1024 * 1024


def per_device(queries, cache_pool, block_scale, block_table, lengths, output_weight):
    seq_count = lax.axis_size("seq")
    group_count = lax.axis_size("grp")
    seq_index = lax.axis_index("seq")
    group_index = lax.axis_index("grp")
    sources = seq_count * group_count
    pool_slots = cache_pool.shape[0]
    key_heads = cache_pool.shape[1]
    block_size = cache_pool.shape[3]
    head_size = cache_pool.shape[4]
    batch_rows, table_width = block_table.shape
    per_group = batch_rows // group_count
    share_blocks = table_width // seq_count
    heads_here = queries.shape[1]
    groups = heads_here // key_heads
    root_scale = 1.0 / math.sqrt(head_size)
    rows = 2 * block_size
    source_index = seq_index * group_count + group_index
    first, second = outgoing_codes(block_table, source_index, pool_slots, group_count, seq_count)
    tall = 2 * rows + scale_rows
    outgoing = pl.pallas_call(
        functools.partial(gather_kernel, group_count, seq_count, pool_slots),
        out_shape=jax.ShapeDtypeStruct((sources, tall, head_size), cache_pool.dtype),
        in_specs=[smem, smem, smem, anywhere],
        out_specs=anywhere,
        scratch_shapes=[
            pltpu.VMEM((sources, tall, head_size), cache_pool.dtype),
            pltpu.SemaphoreType.DMA((2 * sources,)),
            pltpu.SemaphoreType.DMA((sources,)),
        ],
        compiler_params=pltpu.CompilerParams(vmem_limit_bytes=small_grant),
    )(
        first,
        second,
        block_scale.astype(jnp.float32).reshape(-1),
        cache_pool.reshape(pool_slots, rows, head_size),
    )
    arrived = lax.all_to_all(outgoing, both_axes, split_axis=0, concat_axis=0, tiled=True)
    first_place, second_place = arrival_places(
        block_table, seq_index, group_index, pool_slots, group_count, seq_count
    )
    placed, scale_lines = pl.pallas_call(
        place_kernel,
        out_shape=(
            jax.ShapeDtypeStruct((pool_slots, rows, head_size), cache_pool.dtype),
            jax.ShapeDtypeStruct((pool_slots, 128), jnp.float32),
        ),
        in_specs=[smem, smem, anywhere],
        out_specs=(anywhere, vmem),
        scratch_shapes=[
            pltpu.VMEM((sources, tall, head_size), cache_pool.dtype),
            pltpu.SemaphoreType.DMA((sources,)),
            pltpu.SemaphoreType.DMA((2 * sources,)),
        ],
        compiler_params=pltpu.CompilerParams(vmem_limit_bytes=small_grant),
    )(first_place, second_place, arrived)
    decode_cache = placed.reshape(
        per_group, share_blocks, key_heads, 2, block_size, head_size
    )
    decode_scale = (
        scale_lines[:, :2].astype(block_scale.dtype).reshape(per_group, share_blocks, key_heads, 2)
    )
    own_lengths = lax.dynamic_slice_in_dim(lengths, group_index * per_group, per_group)
    block_queries = jnp.broadcast_to(
        queries.reshape(per_group, 1, key_heads, groups, head_size),
        (per_group, share_blocks, key_heads, groups, head_size),
    )
    block_queries = block_queries.reshape(pool_slots, key_heads, groups, head_size)
    block_starts = (
        seq_index * share_blocks + jnp.arange(share_blocks, dtype=jnp.int32)
    ) * block_size
    positions = block_starts[None, :, None] + jnp.arange(block_size, dtype=jnp.int32)[None, None, :]
    live_mask = (positions < own_lengths[:, None, None]).reshape(pool_slots, block_size)
    flat_cache = decode_cache.reshape((pool_slots,) + decode_cache.shape[2:])
    flat_scale = scale_lines[:, :2].reshape(pool_slots, key_heads, 2)
    scores = block_scores(
        block_queries, flat_cache[:, :, 0], flat_scale[:, :, 0], live_mask, root_scale
    )
    request_peak = jnp.max(
        scores.reshape(per_group, share_blocks, key_heads, groups, block_size), axis=(1, 4)
    )
    peak_rows = jnp.broadcast_to(
        request_peak[:, None], (per_group, share_blocks, key_heads, groups)
    )
    peak_rows = peak_rows.reshape(pool_slots, key_heads, groups)
    weight_sum, partial_sum = block_terms(
        scores, peak_rows, live_mask, flat_cache[:, :, 1], flat_scale[:, :, 1]
    )
    request_sum = jnp.sum(weight_sum.reshape(per_group, share_blocks, key_heads, groups), axis=1)
    request_accum = jnp.sum(
        partial_sum.reshape(per_group, share_blocks, key_heads, groups, head_size), axis=1
    )
    peak_all, sum_all, accum_all = joined_all(
        (request_peak, request_sum, request_accum), "seq", combine
    )
    attended = (
        (accum_all / sum_all[..., None])
        .astype(jnp.bfloat16)
        .reshape(per_group, heads_here * head_size)
    )
    partial_out = jnp.dot(
        gather_directly(attended, "grp", 0), output_weight, preferred_element_type=jnp.float32
    )
    summed = sum_at_owner(partial_out, "tp", 0)
    return (summed.astype(jnp.bfloat16), decode_cache, decode_scale)


def solution(mesh):
    placed = (
        P("grp", "tp", None),
        P(("seq", "grp"), "tp", None, None, None),
        P(("seq", "grp"), "tp", None),
        P(),
        P(),
        P("tp", ("seq", "grp")),
    )
    return jax.shard_map(
        per_device,
        mesh=mesh,
        in_specs=placed,
        out_specs=(
            P("tp", ("seq", "grp")),
            P("grp", "seq", "tp", None, None, None),
            P("grp", "seq", "tp", None),
        ),
        check_vma=False,
    )
```

```python
import functools
import math

import jax
import jax.numpy as jnp
from jax import lax
from jax.experimental import pallas as pl
from jax.experimental.pallas import tpu as pltpu
from jax.sharding import PartitionSpec as P

absent_score = -1e30
both_axes = ("seq", "grp")
far = 1 << 20
scale_rows = 8


def outgoing_codes(block_table, source, slots, groups, ranges):
    rows, width = block_table.shape
    per_group, span = rows // groups, width // ranges
    table = block_table.reshape(groups, per_group, width)
    column = lax.broadcasted_iota(jnp.int32, table.shape, 2)
    row = lax.broadcasted_iota(jnp.int32, table.shape, 1)
    code = (row * span + column % span) * slots + table % slots
    mine = (table // slots == source)[:, :, None, :] & (
        (column // span)[:, :, None, :] == jnp.arange(ranges, dtype=jnp.int32)[None, None, :, None]
    )
    code = jnp.broadcast_to(code[:, :, None, :], mine.shape)
    return (
        jnp.min(jnp.where(mine, code, far), axis=(1, 3)),
        jnp.max(jnp.where(mine, code, -1), axis=(1, 3)),
    )


def arrival_places(block_table, seq_index, group_index, slots, groups, ranges):
    rows, width = block_table.shape
    per_group, span = rows // groups, width // ranges
    own = lax.dynamic_slice(
        block_table, (group_index * per_group, seq_index * span), (per_group, span)
    )
    source = (own // slots)[None]
    place = lax.broadcasted_iota(jnp.int32, (1, per_group, span), 1) * span
    place = place + lax.broadcasted_iota(jnp.int32, (1, per_group, span), 2)
    here = source == jnp.arange(groups * ranges, dtype=jnp.int32)[:, None, None]
    return (
        jnp.min(jnp.where(here, place, far), axis=(1, 2)),
        jnp.max(jnp.where(here, place, -1), axis=(1, 2)),
    )


def place_kernel(first, second, arrived, cache, scale, held, in_sem, out_sem):
    sources = arrived.shape[0]
    rows = cache.shape[1]
    copies = []
    for d in range(sources):
        copy = pltpu.make_async_copy(arrived.at[d], held.at[d], in_sem.at[d])
        copy.start()
        copies.append(copy)
    sent = []
    for d in range(sources):
        copies[d].wait()
        for k, places in enumerate((first, second)):
            copy = pltpu.make_async_copy(
                held.at[d, pl.ds(k * rows, rows)], cache.at[places[d]], out_sem.at[2 * d + k]
            )
            copy.start()
            sent.append(copy)
        tile = held[d, pl.ds(2 * rows, scale_rows)].astype(jnp.float32)
        for k, places in enumerate((first, second)):
            scale[pl.ds(places[d], 1), :] = tile[k : k + 1]
    for copy in sent:
        copy.wait()


def gather_kernel(groups, ranges, slots, codes, scales, pool, out, held, in_sem, out_sem):
    rows = pool.shape[1]
    copies = []
    for s in range(ranges):
        for g in range(groups):
            d = s * groups + g
            for k in range(2):
                copy = pltpu.make_async_copy(
                    pool.at[codes[k, g, s] & (slots - 1)],
                    held.at[d, pl.ds(k * rows, rows)],
                    in_sem.at[2 * d + k],
                )
                copy.start()
                copies.append(copy)
    row = lax.broadcasted_iota(jnp.int32, (scale_rows, 128), 0)
    lane = lax.broadcasted_iota(jnp.int32, (scale_rows, 128), 1)
    for s in range(ranges):
        for g in range(groups):
            d = s * groups + g
            one, two = (codes[k, g, s] & (slots - 1) for k in range(2))
            keys = jnp.where(row == 0, scales[2 * one], scales[2 * two])
            values = jnp.where(row == 0, scales[2 * one + 1], scales[2 * two + 1])
            held[d, pl.ds(2 * rows, scale_rows)] = jnp.where(lane == 0, keys, values).astype(
                held.dtype
            )
    sent = []
    for d in range(groups * ranges):
        for k in range(2):
            copies[2 * d + k].wait()
        copy = pltpu.make_async_copy(held.at[d], out.at[d], out_sem.at[d])
        copy.start()
        sent.append(copy)
    for copy in sent:
        copy.wait()


def stat_rows(peak, total, half):
    row = lax.broadcasted_iota(jnp.int32, (half, 128), 0)
    lane = lax.broadcasted_iota(jnp.int32, (half, 128), 1)
    peak_row = jnp.sum(jnp.where(row == lane, peak, 0.0), axis=0, keepdims=True)
    total_row = jnp.sum(jnp.where(row == lane, total, 0.0), axis=0, keepdims=True)
    line = lax.broadcasted_iota(jnp.int32, (8, 128), 0)
    return jnp.where(line == 0, peak_row, jnp.where(line == 1, total_row, 0.0))


def as_column(line, half):
    row = lax.broadcasted_iota(jnp.int32, (half, 128), 0)
    lane = lax.broadcasted_iota(jnp.int32, (half, 128), 1)
    return jnp.sum(jnp.where(row == lane, line, 0.0), axis=1, keepdims=True)


def attend_kernel(
    sizes, codes, scales, lens, where_at, own_q, other_q, blocks, keep, give, held, peaks, totals, sem
):
    groups, ranges, slots, span, root_scale = sizes
    cores = 2
    chips = groups // cores
    bits, span_bits = slots.bit_length() - 1, span.bit_length() - 1
    size = blocks.shape[2]
    heads = own_q.shape[1] // 2
    chip, core = where_at[0], where_at[1]
    order = [(flip, k) for flip in range(cores) for k in range(chips)]
    copies = []
    for i, (flip, k) in enumerate(order):
        g = cores * ((chip - k) & (chips - 1)) + (core ^ flip)
        for s in range(ranges):
            n = i * ranges + s
            copy = pltpu.make_async_copy(
                blocks.at[s * groups + g, pl.ds(0, 4 * size)], held.at[n], sem.at[n]
            )
            copy.start()
            copies.append(copy)
    line = lax.broadcasted_iota(jnp.int32, (2 * heads, size), 0)
    lane = lax.broadcasted_iota(jnp.int32, (2 * heads, size), 1)
    for i, (flip, k) in enumerate(order):
        at = (chip - k) & (chips - 1)
        g = cores * at + (core ^ flip)
        query = (other_q if flip else own_q)[k]
        scored, lives, values = [], [], []
        for s in range(ranges):
            copies[i * ranges + s].wait()
            for kk in range(2):
                code = codes[kk, g, s]
                slot, place = code & (slots - 1), code >> bits
                member, column = place >> span_bits, place & (span - 1)
                limit = lens[2 * g + member] - (s * span + column) * size
                keys = held[i * ranges + s, pl.ds(2 * kk * size, size)]
                score = lax.dot_general(
                    query, keys, (((1,), (1,)), ((), ())), preferred_element_type=jnp.float32
                )
                low = member * heads
                live = (line >= low) & (line < low + heads) & (lane < limit)
                scored.append(
                    jnp.where(live, score * scales[2 * slot] * root_scale, absent_score)
                )
                lives.append(live)
                values.append(scales[2 * slot + 1])
        peak = functools.reduce(jnp.maximum, scored)
        peak = jnp.max(peak, axis=1, keepdims=True)
        total, summed = 0.0, 0.0
        for n, (score, live, value) in enumerate(zip(scored, lives, values)):
            weight = jnp.where(live, jnp.exp(score - peak), 0.0)
            total = total + weight
            rows = held[i * ranges + n // 2, pl.ds((2 * (n % 2) + 1) * size, size)]
            summed = summed + jnp.dot(
                (weight * value).astype(jnp.bfloat16), rows, preferred_element_type=jnp.float32
            )
        total = jnp.sum(total, axis=1, keepdims=True)
        to = pl.ds(pl.multiple_of(at * 2 * heads, 2 * heads), 2 * heads)
        (give if flip else keep)[to, :] = summed
        peaks[flip, to, :] = jnp.broadcast_to(peak, (2 * heads, 128))
        totals[flip, to, :] = jnp.broadcast_to(total, (2 * heads, 128))
    half = chips * 2 * heads
    for flip, out in enumerate((keep, give)):
        out[pl.ds(half, 8), :] = stat_rows(peaks[flip], totals[flip], half)


def merged(a, b):
    half = a.shape[0] - 8
    peak_a, peak_b = a[pl.ds(half, 1), :], b[pl.ds(half, 1), :]
    peak = jnp.maximum(peak_a, peak_b)
    factor_a, factor_b = jnp.exp(peak_a - peak), jnp.exp(peak_b - peak)
    total = a[pl.ds(half + 1, 1), :] * factor_a + b[pl.ds(half + 1, 1), :] * factor_b
    summed = a[pl.ds(0, half), :] * as_column(factor_a, half) + b[
        pl.ds(0, half), :
    ] * as_column(factor_b, half)
    return peak, total, summed


def merge_kernel(a, b, out):
    half = a.shape[0] - 8
    peak, total, summed = merged(a, b)
    out[pl.ds(0, half), :] = summed
    line = lax.broadcasted_iota(jnp.int32, (8, 128), 0)
    out[pl.ds(half, 8), :] = jnp.where(line == 0, peak, jnp.where(line == 1, total, 0.0))


def finish_kernel(a, b, out):
    _, total, summed = merged(a, b)
    out[...] = summed / as_column(total, out.shape[0])


def project_kernel(where_at, own, other, weight, out):
    size = own.shape[1]
    heads = weight.shape[0] // size
    lines = own.shape[0] // heads
    summed = 0.0
    for k in range(heads):
        rows = jnp.concatenate(
            [ref[pl.ds(k, lines, stride=heads), :] for ref in (own, other)], axis=0
        )
        summed = summed + jnp.dot(
            rows.astype(jnp.bfloat16),
            weight[pl.ds(k * size, size), :],
            preferred_element_type=jnp.float32,
        )
    core = where_at[1]
    for at in range(lines // 2):
        out[2 * at + core] = summed[2 * at : 2 * at + 2]
        out[2 * at + 1 - core] = summed[lines + 2 * at : lines + 2 * at + 2]


tight = pltpu.CompilerParams(vmem_limit_bytes=4 * 1024 * 1024)
wide = pltpu.CompilerParams(vmem_limit_bytes=60 * 1024 * 1024)
smem = pl.BlockSpec(memory_space=pltpu.SMEM)
vmem = pl.BlockSpec(memory_space=pltpu.VMEM)
anywhere = pl.BlockSpec(memory_space=pl.ANY)
all_axes = ("seq", "tp", "grp")


def flipped(array, y=0, z=0, x=0, core=0):
    tps, grps = lax.axis_size("tp"), lax.axis_size("grp")
    pairs = []
    for i in range(lax.axis_size("seq") * tps * grps):
        a, b, c = i // (tps * grps), i // grps % tps, i % grps
        pairs.append((i, ((a ^ y) * tps + (b ^ z)) * grps + (c ^ (2 * x + core))))
    return lax.ppermute(array, all_axes, pairs)


def merge(a, b, kernel=merge_kernel, rows=None):
    return pl.pallas_call(
        kernel,
        out_shape=jax.ShapeDtypeStruct((rows or a.shape[0], a.shape[1]), a.dtype),
        in_specs=[vmem, vmem],
        out_specs=vmem,
        compiler_params=tight,
    )(a, b)


def per_device(queries, cache_pool, block_scale, block_table, lengths, output_weight):
    seq_count = lax.axis_size("seq")
    group_count = lax.axis_size("grp")
    seq_index = lax.axis_index("seq")
    group_index = lax.axis_index("grp")
    sources = seq_count * group_count
    chips = group_count // 2
    pool_slots = cache_pool.shape[0]
    key_heads = cache_pool.shape[1]
    block_size = cache_pool.shape[3]
    head_size = cache_pool.shape[4]
    batch_rows, table_width = block_table.shape
    per_group = batch_rows // group_count
    share_blocks = table_width // seq_count
    heads_here = queries.shape[1]
    root_scale = 1.0 / math.sqrt(head_size)
    rows = 2 * block_size
    source_index = seq_index * group_count + group_index
    where_at = jnp.stack([group_index // 2, group_index % 2]).astype(jnp.int32)

    flat_queries = queries.reshape(per_group * heads_here, head_size)
    own_q = [flat_queries]
    for k in range(1, chips):
        turn = [(i, (i + 2 * k) % group_count) for i in range(group_count)]
        own_q.append(lax.ppermute(flat_queries, "grp", turn))
    own_q = jnp.stack(own_q)

    codes = jnp.stack(
        outgoing_codes(block_table, source_index, pool_slots, group_count, seq_count)
    )
    flat_scales = block_scale.astype(jnp.float32).reshape(-1)
    tall = 2 * rows + scale_rows
    outgoing = pl.pallas_call(
        functools.partial(gather_kernel, group_count, seq_count, pool_slots),
        out_shape=jax.ShapeDtypeStruct((sources, tall, head_size), cache_pool.dtype),
        in_specs=[smem, smem, anywhere],
        out_specs=anywhere,
        scratch_shapes=[
            pltpu.VMEM((sources, tall, head_size), cache_pool.dtype),
            pltpu.SemaphoreType.DMA((2 * sources,)),
            pltpu.SemaphoreType.DMA((sources,)),
        ],
        compiler_params=wide,
    )(codes, flat_scales, cache_pool.reshape(pool_slots, rows, head_size))
    outgoing, own_q = lax.optimization_barrier((outgoing, own_q))
    other_q = flipped(own_q, core=1)
    arrived = lax.all_to_all(outgoing, both_axes, split_axis=0, concat_axis=0, tiled=True)

    half = chips * per_group * heads_here
    line_shape = jax.ShapeDtypeStruct((half + 8, head_size), jnp.float32)
    keep, give = pl.pallas_call(
        functools.partial(
            attend_kernel, (group_count, seq_count, pool_slots, share_blocks, root_scale)
        ),
        out_shape=(line_shape, line_shape),
        in_specs=[smem, smem, smem, smem, vmem, vmem, anywhere],
        out_specs=(vmem, vmem),
        scratch_shapes=[
            pltpu.VMEM((sources, 2 * rows, head_size), cache_pool.dtype),
            pltpu.VMEM((2, half, 128), jnp.float32),
            pltpu.VMEM((2, half, 128), jnp.float32),
            pltpu.SemaphoreType.DMA((sources,)),
        ],
        compiler_params=wide,
    )(codes, flat_scales, lengths, where_at, own_q, other_q, outgoing)
    lines = merge(keep, flipped(give, core=1))
    steps = [{"x": 1}, {"x": 2}, {"y": 1}, {"y": 2}]
    for n, step in enumerate(steps):
        across = flipped(lines, z=1)
        beside = flipped(lines, z=1, **step)
        if n < len(steps) - 1:
            lines = merge(across, beside)
        else:
            lines = merge(across, beside, finish_kernel, half)
    partial_out = pl.pallas_call(
        project_kernel,
        out_shape=jax.ShapeDtypeStruct(
            (group_count, per_group, output_weight.shape[1]), jnp.float32
        ),
        in_specs=[smem, vmem, vmem, vmem],
        out_specs=vmem,
        compiler_params=tight,
    )(where_at, lines, flipped(lines, core=1), output_weight)
    partial_out, _ = lax.optimization_barrier((partial_out, arrived))
    summed = lax.all_to_all(partial_out, "tp", split_axis=0, concat_axis=0, tiled=True).sum(axis=0)

    first_place, second_place = arrival_places(
        block_table, seq_index, group_index, pool_slots, group_count, seq_count
    )
    placed, scale_lines = pl.pallas_call(
        place_kernel,
        out_shape=(
            jax.ShapeDtypeStruct((pool_slots, rows, head_size), cache_pool.dtype),
            jax.ShapeDtypeStruct((pool_slots, 128), jnp.float32),
        ),
        in_specs=[smem, smem, anywhere],
        out_specs=(anywhere, vmem),
        scratch_shapes=[
            pltpu.VMEM((sources, tall, head_size), cache_pool.dtype),
            pltpu.SemaphoreType.DMA((sources,)),
            pltpu.SemaphoreType.DMA((2 * sources,)),
        ],
        compiler_params=wide,
    )(first_place, second_place, arrived)
    decode_cache = placed.reshape(
        per_group, share_blocks, key_heads, 2, block_size, head_size
    )
    decode_scale = (
        scale_lines[:, :2].astype(block_scale.dtype).reshape(per_group, share_blocks, key_heads, 2)
    )
    return (summed.astype(jnp.bfloat16), decode_cache, decode_scale)


def solution(mesh):
    placed = (
        P("grp", "tp", None),
        P(("seq", "grp"), "tp", None, None, None),
        P(("seq", "grp"), "tp", None),
        P(),
        P(),
        P("tp", ("seq", "grp")),
    )
    return jax.shard_map(
        per_device,
        mesh=mesh,
        in_specs=placed,
        out_specs=(
            P("tp", ("seq", "grp")),
            P("grp", "seq", "tp", None, None, None),
            P("grp", "seq", "tp", None),
        ),
        check_vma=False,
    )
```

```python
import functools
import math

import jax
import jax.numpy as jnp
from jax import lax
from jax.experimental import pallas as pl
from jax.experimental.pallas import tpu as pltpu
from jax.sharding import PartitionSpec as P

absent_score = -1e30
both_axes = ("seq", "grp")
all_axes = ("seq", "tp", "grp")
far = 1 << 20
scale_rows = 8


def arrival_places(block_table, seq_index, group_index, slots, groups, ranges):
    rows, width = block_table.shape
    per_group, span = rows // groups, width // ranges
    own = lax.dynamic_slice(
        block_table, (group_index * per_group, seq_index * span), (per_group, span)
    )
    source = (own // slots)[None]
    place = lax.broadcasted_iota(jnp.int32, (1, per_group, span), 1) * span
    place = place + lax.broadcasted_iota(jnp.int32, (1, per_group, span), 2)
    here = source == jnp.arange(groups * ranges, dtype=jnp.int32)[:, None, None]
    return (
        jnp.min(jnp.where(here, place, far), axis=(1, 2)),
        jnp.max(jnp.where(here, place, -1), axis=(1, 2)),
    )


def code_at(codes, ranges, k, g, s):
    return codes[2 * g, k * ranges + s]


def gather_kernel(
    sizes, table_in, scales_in, pool, out, codes_out, scales_out, table, scales, codes, scale_lines,
    held, tiles, codes_s, scales_s, load, store, side
):
    groups, ranges, slots, span = sizes
    rows = pool.shape[1]
    loads = []
    step = slots // 8
    for i in range(8):
        part = pl.ds(i * step, step)
        loads.append(pltpu.make_async_copy(pool.at[part], held.at[part], load.at[i]))
    small = [
        pltpu.make_async_copy(table_in, table, side.at[3]),
        pltpu.make_async_copy(scales_in, scales, side.at[4]),
    ]
    for copy in small + loads[:4]:
        copy.start()
    for copy in small:
        copy.wait()
    source = lax.axis_index("seq") * groups + lax.axis_index("grp")
    entry = table[...]
    row = lax.broadcasted_iota(jnp.int32, entry.shape, 0)
    lane = lax.broadcasted_iota(jnp.int32, entry.shape, 1)
    code = ((row & 1) * span + (lane & (span - 1))) * slots + (entry & (slots - 1))
    code = code.astype(jnp.float32)
    mine = (entry >> (slots.bit_length() - 1)) == source
    found = jnp.full(entry.shape, float(far))
    for s in range(ranges):
        here = mine & ((lane >> (span.bit_length() - 1)) == s)
        for k, value in enumerate((code, -code)):
            least = jnp.min(jnp.where(here, value, float(far)), axis=1, keepdims=True)
            found = jnp.where(lane == k * ranges + s, least, found)
    found = jnp.minimum(found, pltpu.roll(found, entry.shape[0] - 1, 0))
    codes[...] = jnp.where(lane < ranges, found, -found).astype(jnp.int32)
    scale_lines[...] = jnp.zeros(scale_lines.shape, jnp.float32)
    scale_lines[pl.ds(0, 2), pl.ds(0, slots)] = scales[...].astype(jnp.float32)
    for copy in loads[4:]:
        copy.start()
    sides = [
        pltpu.make_async_copy(codes, codes_s, side.at[0]),
        pltpu.make_async_copy(scale_lines, scales_s, side.at[1]),
        pltpu.make_async_copy(codes, codes_out, side.at[5]),
        pltpu.make_async_copy(scale_lines, scales_out, side.at[6]),
    ]
    for copy in sides:
        copy.start()
    for copy in sides[:2]:
        copy.wait()
    row = lax.broadcasted_iota(jnp.int32, (scale_rows, 128), 0)
    lane = lax.broadcasted_iota(jnp.int32, (scale_rows, 128), 1)
    chosen = []
    for s in range(ranges):
        for g in range(groups):
            one, two = (code_at(codes_s, ranges, k, g, s) & (slots - 1) for k in range(2))
            chosen += [one, two]
            keys = jnp.where(row == 0, scales_s[0, one], scales_s[0, two])
            values = jnp.where(row == 0, scales_s[1, one], scales_s[1, two])
            tiles[s * groups + g] = jnp.where(lane == 0, keys, values).astype(tiles.dtype)
    for copy in loads:
        copy.wait()
    stores = []
    for n, slot in enumerate(chosen):
        stores.append(
            pltpu.make_async_copy(
                held.at[slot], out.at[n // 2, pl.ds(n % 2 * rows, rows)], store.at[n]
            )
        )
        stores[-1].start()
    stores.append(
        pltpu.make_async_copy(tiles, out.at[:, pl.ds(2 * rows, scale_rows)], side.at[2])
    )
    stores[-1].start()
    for copy in stores + sides[2:]:
        copy.wait()


def place_kernel(places_in, arrived, cache, scale_out, places, scale, held, lines, load, store, side):
    sources = arrived.shape[0]
    rows = cache.shape[1]
    step = sources // 8
    loads = []
    for i in range(8):
        part = pl.ds(i * step, step)
        loads.append(pltpu.make_async_copy(arrived.at[part], held.at[part], load.at[i]))
        loads[-1].start()
    copy = pltpu.make_async_copy(places_in, places, side.at[0])
    copy.start()
    copy.wait()
    stores = []
    for d in range(sources):
        if d % step == 0:
            loads[d // step].wait()
        for k in range(2):
            stores.append(
                pltpu.make_async_copy(
                    held.at[d, pl.ds(k * rows, rows)], cache.at[places[k, d]], store.at[2 * d + k]
                )
            )
            stores[-1].start()
    for d in range(sources):
        tile = held[d, pl.ds(2 * rows, scale_rows)].astype(jnp.float32)
        for k in range(2):
            lines[pl.ds(places[k, d], 1), :] = tile[k : k + 1]
    pick = lax.broadcasted_iota(jnp.int32, (8, 128), 0) == lax.broadcasted_iota(
        jnp.int32, (8, 128), 1
    )
    pick = jnp.where(pick, 1.0, 0.0).astype(jnp.bfloat16)
    members, _, span = scale.shape
    for b in range(members):
        turned = lax.dot_general(
            pick,
            lines[pl.ds(b * span, span), :].astype(jnp.bfloat16),
            (((1,), (1,)), ((), ())),
            preferred_element_type=jnp.float32,
        )
        scale[b] = turned[:2].astype(scale.dtype)
    stores.append(pltpu.make_async_copy(scale, scale_out, side.at[1]))
    stores[-1].start()
    for copy in stores:
        copy.wait()


def stat_rows(peak, total, half):
    row = lax.broadcasted_iota(jnp.int32, (half, 128), 0)
    lane = lax.broadcasted_iota(jnp.int32, (half, 128), 1)
    peak_row = jnp.sum(jnp.where(row == lane, peak, 0.0), axis=0, keepdims=True)
    total_row = jnp.sum(jnp.where(row == lane, total, 0.0), axis=0, keepdims=True)
    line = lax.broadcasted_iota(jnp.int32, (8, 128), 0)
    return jnp.where(line == 0, peak_row, jnp.where(line == 1, total_row, 0.0))


def as_column(line, half):
    row = lax.broadcasted_iota(jnp.int32, (half, 128), 0)
    lane = lax.broadcasted_iota(jnp.int32, (half, 128), 1)
    return jnp.sum(jnp.where(row == lane, line, 0.0), axis=1, keepdims=True)


def attend_kernel(
    sizes, codes, scales, lens, own_q, other_q, blocks, keep, give, held, peaks, totals, sem
):
    groups, ranges, slots, span, root_scale = sizes
    cores = 2
    chips = groups // cores
    bits, span_bits = slots.bit_length() - 1, span.bit_length() - 1
    size = blocks.shape[2]
    heads = own_q.shape[1] // 2
    group = lax.axis_index("grp")
    chip, core = group >> 1, group & 1
    order = [(flip, k) for flip in range(cores) for k in range(chips)]
    copies = []
    for i, (flip, k) in enumerate(order):
        g = cores * ((chip - k) & (chips - 1)) + (core ^ flip)
        for s in range(ranges):
            n = i * ranges + s
            copy = pltpu.make_async_copy(
                blocks.at[s * groups + g, pl.ds(0, 4 * size)], held.at[n], sem.at[n]
            )
            copy.start()
            copies.append(copy)
    line = lax.broadcasted_iota(jnp.int32, (2 * heads, size), 0)
    lane = lax.broadcasted_iota(jnp.int32, (2 * heads, size), 1)
    parts = []
    for copy in copies:
        copy.wait()
    for i, (flip, k) in enumerate(order):
        at = (chip - k) & (chips - 1)
        g = cores * at + (core ^ flip)
        query = (other_q if flip else own_q)[k]
        scored, lives, values = [], [], []
        for s in range(ranges):
            for kk in range(2):
                code = code_at(codes, ranges, kk, g, s)
                slot, place = code & (slots - 1), code >> bits
                member, column = place >> span_bits, place & (span - 1)
                limit = lens[2 * g + member] - (s * span + column) * size
                keys = held[i * ranges + s, pl.ds(2 * kk * size, size)]
                score = lax.dot_general(
                    query, keys, (((1,), (1,)), ((), ())), preferred_element_type=jnp.float32
                )
                low = member * heads
                live = (line >= low) & (line < low + heads) & (lane < limit)
                scored.append(
                    jnp.where(live, score * scales[0, slot] * root_scale, absent_score)
                )
                lives.append(live)
                values.append(scales[1, slot])
        peak = functools.reduce(jnp.maximum, scored)
        peak = jnp.max(peak, axis=1, keepdims=True)
        parts.append((at, flip, peak, scored, lives, values))
    for i, (at, flip, peak, scored, lives, values) in enumerate(parts):
        total, summed = 0.0, 0.0
        for n, (score, live, value) in enumerate(zip(scored, lives, values)):
            weight = jnp.where(live, jnp.exp(score - peak), 0.0)
            total = total + weight
            rows = held[i * ranges + n // 2, pl.ds((2 * (n % 2) + 1) * size, size)]
            summed = summed + jnp.dot(
                (weight * value).astype(jnp.bfloat16), rows, preferred_element_type=jnp.float32
            )
        total = jnp.sum(total, axis=1, keepdims=True)
        to = pl.ds(pl.multiple_of(at * 2 * heads, 2 * heads), 2 * heads)
        (give if flip else keep)[to, :] = summed
        peaks[flip, to, :] = jnp.broadcast_to(peak, (2 * heads, 128))
        totals[flip, to, :] = jnp.broadcast_to(total, (2 * heads, 128))
    half = chips * 2 * heads
    for flip, out in enumerate((keep, give)):
        out[pl.ds(half, 8), :] = stat_rows(peaks[flip], totals[flip], half)


def merged(a, b):
    half = a.shape[0] - 8
    peak_a, peak_b = a[pl.ds(half, 1), :], b[pl.ds(half, 1), :]
    peak = jnp.maximum(peak_a, peak_b)
    factor_a, factor_b = jnp.exp(peak_a - peak), jnp.exp(peak_b - peak)
    total = a[pl.ds(half + 1, 1), :] * factor_a + b[pl.ds(half + 1, 1), :] * factor_b
    summed = a[pl.ds(0, half), :] * as_column(factor_a, half) + b[
        pl.ds(0, half), :
    ] * as_column(factor_b, half)
    return peak, total, summed


def merge_kernel(a, b, out):
    half = a.shape[0] - 8
    peak, total, summed = merged(a, b)
    out[pl.ds(0, half), :] = summed
    line = lax.broadcasted_iota(jnp.int32, (8, 128), 0)
    out[pl.ds(half, 8), :] = jnp.where(line == 0, peak, jnp.where(line == 1, total, 0.0))


def finish_kernel(a, b, out):
    _, total, summed = merged(a, b)
    out[...] = summed / as_column(total, out.shape[0])


def project_kernel(own, other, weight, keep, give, slots):
    size = own.shape[1]
    heads = weight.shape[0] // size
    lines = own.shape[0] // heads
    summed = 0.0
    for k in range(heads):
        rows = jnp.concatenate(
            [ref[pl.ds(k, lines, stride=heads), :] for ref in (own, other)], axis=0
        )
        summed = summed + jnp.dot(
            rows.astype(jnp.bfloat16),
            weight[pl.ds(k * size, size), :],
            preferred_element_type=jnp.float32,
        )
    core = lax.axis_index("grp") & 1
    here = lax.axis_index("tp")
    count = keep.shape[0]
    for flip in range(2):
        for at in range(lines // 2):
            j = (2 * at + (core ^ flip)) ^ here
            first = flip * lines + 2 * at
            slots[(j >> 1) + count * (j & 1)] = summed[first : first + 2]
    keep[...] = slots[pl.ds(0, count)]
    give[...] = slots[pl.ds(count, count)]


def split_kernel(keep, came, *outs):
    for i, out in enumerate(outs):
        out[...] = keep[i] + came[i]


def add_kernel(*refs):
    *terms, out = refs
    total = terms[0][...]
    for term in terms[1:]:
        total = total + term[...]
    out[...] = total.astype(out.dtype)


tight = pltpu.CompilerParams(vmem_limit_bytes=4 * 1024 * 1024)
wide = pltpu.CompilerParams(vmem_limit_bytes=60 * 1024 * 1024)
smem = pl.BlockSpec(memory_space=pltpu.SMEM)
vmem = pl.BlockSpec(memory_space=pltpu.VMEM)
hbm = pl.BlockSpec(memory_space=pltpu.HBM)


def flipped(array, y=0, z=0, x=0, core=0):
    tps, grps = lax.axis_size("tp"), lax.axis_size("grp")
    pairs = []
    for i in range(lax.axis_size("seq") * tps * grps):
        a, b, c = i // (tps * grps), i // grps % tps, i % grps
        pairs.append((i, ((a ^ y) * tps + (b ^ z)) * grps + (c ^ (2 * x + core))))
    return lax.ppermute(array, all_axes, pairs)


def merge(a, b, kernel=merge_kernel, rows=None):
    return pl.pallas_call(
        kernel,
        out_shape=jax.ShapeDtypeStruct((rows or a.shape[0], a.shape[1]), a.dtype),
        in_specs=[vmem, vmem],
        out_specs=vmem,
        compiler_params=tight,
    )(a, b)


def per_device(queries, cache_pool, block_scale, block_table, lengths, output_weight):
    seq_count = lax.axis_size("seq")
    group_count = lax.axis_size("grp")
    tp_count = lax.axis_size("tp")
    sources = seq_count * group_count
    chips = group_count // 2
    pool_slots = cache_pool.shape[0]
    key_heads = cache_pool.shape[1]
    block_size = cache_pool.shape[3]
    head_size = cache_pool.shape[4]
    batch_rows, table_width = block_table.shape
    per_group = batch_rows // group_count
    share_blocks = table_width // seq_count
    heads_here = queries.shape[1]
    out_width = output_weight.shape[1]
    root_scale = 1.0 / math.sqrt(head_size)
    rows = 2 * block_size

    flat_queries = queries.reshape(per_group * heads_here, head_size)
    own_q = [flat_queries]
    for k in range(1, chips):
        turn = [(i, (i + 2 * k) % group_count) for i in range(group_count)]
        own_q.append(lax.ppermute(flat_queries, "grp", turn))

    tall = 2 * rows + scale_rows
    outgoing, codes, scale_lines = pl.pallas_call(
        functools.partial(gather_kernel, (group_count, seq_count, pool_slots, share_blocks)),
        out_shape=(
            jax.ShapeDtypeStruct((sources, tall, head_size), cache_pool.dtype),
            jax.ShapeDtypeStruct(block_table.shape, jnp.int32),
            jax.ShapeDtypeStruct((8, 128), jnp.float32),
        ),
        in_specs=[hbm, hbm, hbm],
        out_specs=(hbm, hbm, hbm),
        scratch_shapes=[
            pltpu.VMEM(block_table.shape, jnp.int32),
            pltpu.VMEM((2, pool_slots), block_scale.dtype),
            pltpu.VMEM(block_table.shape, jnp.int32),
            pltpu.VMEM((8, 128), jnp.float32),
            pltpu.VMEM((pool_slots, rows, head_size), cache_pool.dtype),
            pltpu.VMEM((sources, scale_rows, 128), cache_pool.dtype),
            pltpu.SMEM(block_table.shape, jnp.int32),
            pltpu.SMEM((8, 128), jnp.float32),
            pltpu.SemaphoreType.DMA((8,)),
            pltpu.SemaphoreType.DMA((2 * sources,)),
            pltpu.SemaphoreType.DMA((7,)),
        ],
        compiler_params=wide,
    )(
        block_table,
        block_scale.reshape(pool_slots, 2).T,
        cache_pool.reshape(pool_slots, rows, head_size),
    )
    outgoing, own_q = lax.optimization_barrier((outgoing, own_q))
    own_q = jnp.stack(own_q)
    other_q = flipped(own_q, core=1)
    arrived = lax.all_to_all(outgoing, both_axes, split_axis=0, concat_axis=0, tiled=True)

    half = chips * per_group * heads_here
    line_shape = jax.ShapeDtypeStruct((half + 8, head_size), jnp.float32)
    keep, give = pl.pallas_call(
        functools.partial(
            attend_kernel, (group_count, seq_count, pool_slots, share_blocks, root_scale)
        ),
        out_shape=(line_shape, line_shape),
        in_specs=[smem, smem, smem, vmem, vmem, hbm],
        out_specs=(vmem, vmem),
        scratch_shapes=[
            pltpu.VMEM((sources, 2 * rows, head_size), cache_pool.dtype),
            pltpu.VMEM((2, half, 128), jnp.float32),
            pltpu.VMEM((2, half, 128), jnp.float32),
            pltpu.SemaphoreType.DMA((sources,)),
        ],
        compiler_params=wide,
    )(codes, scale_lines, lengths, own_q, other_q, outgoing)
    lines = merge(keep, flipped(give, core=1))
    steps = [{"x": 1}, {"x": 2}, {"y": 1}, {"y": 2}]
    for n, step in enumerate(steps):
        across = flipped(lines, z=1)
        beside = flipped(lines, z=1, **step)
        if n < len(steps) - 1:
            lines = merge(across, beside)
        else:
            lines = merge(across, beside, finish_kernel, half)
    places = jnp.stack(
        arrival_places(
            block_table,
            lax.axis_index("seq"),
            lax.axis_index("grp"),
            pool_slots,
            group_count,
            seq_count,
        )
    )
    other_lines, places = lax.optimization_barrier((flipped(lines, core=1), places))
    pair_shape = jax.ShapeDtypeStruct((tp_count // 2, per_group, out_width), jnp.float32)
    keep, give = pl.pallas_call(
        project_kernel,
        out_shape=(pair_shape, pair_shape),
        in_specs=[vmem, vmem, vmem],
        out_specs=(vmem, vmem),
        scratch_shapes=[pltpu.VMEM((tp_count, per_group, out_width), jnp.float32)],
        compiler_params=tight,
    )(lines, other_lines, output_weight)
    share = jax.ShapeDtypeStruct((per_group, out_width), jnp.float32)
    shares = pl.pallas_call(
        split_kernel,
        out_shape=(share,) * (tp_count // 2),
        in_specs=[vmem, vmem],
        out_specs=(vmem,) * (tp_count // 2),
        compiler_params=tight,
    )(keep, flipped(give, z=1))
    terms = [shares[0]] + [flipped(shares[i], z=2 * i) for i in range(1, tp_count // 2)]
    placed, scales = pl.pallas_call(
        place_kernel,
        out_shape=(
            jax.ShapeDtypeStruct((pool_slots, rows, head_size), cache_pool.dtype),
            jax.ShapeDtypeStruct((per_group, 2, share_blocks), block_scale.dtype),
        ),
        in_specs=[hbm, hbm],
        out_specs=(hbm, hbm),
        scratch_shapes=[
            pltpu.SMEM((2, sources), jnp.int32),
            pltpu.VMEM((per_group, 2, share_blocks), block_scale.dtype),
            pltpu.VMEM((sources, tall, head_size), cache_pool.dtype),
            pltpu.VMEM((pool_slots, 128), jnp.float32),
            pltpu.SemaphoreType.DMA((8,)),
            pltpu.SemaphoreType.DMA((2 * sources,)),
            pltpu.SemaphoreType.DMA((2,)),
        ],
        compiler_params=wide,
    )(places, arrived)
    terms, scales = lax.optimization_barrier((terms, scales))
    summed = pl.pallas_call(
        add_kernel,
        out_shape=jax.ShapeDtypeStruct((per_group, out_width), jnp.bfloat16),
        in_specs=[vmem] * len(terms),
        out_specs=vmem,
        compiler_params=tight,
    )(*terms)
    decode_cache = placed.reshape(
        per_group, share_blocks, key_heads, 2, block_size, head_size
    )
    decode_scale = scales.transpose(0, 2, 1).reshape(per_group, share_blocks, key_heads, 2)
    return (summed, decode_cache, decode_scale)


def solution(mesh):
    placed = (
        P("grp", "tp", None),
        P(("seq", "grp"), "tp", None, None, None),
        P(("seq", "grp"), "tp", None),
        P(),
        P(),
        P("tp", ("seq", "grp")),
    )
    return jax.shard_map(
        per_device,
        mesh=mesh,
        in_specs=placed,
        out_specs=(
            P("tp", ("seq", "grp")),
            P("grp", "seq", "tp", None, None, None),
            P("grp", "seq", "tp", None),
        ),
        check_vma=False,
    )
```

```python
import functools
import math

import jax
import jax.numpy as jnp
from jax import lax
from jax.experimental import pallas as pl
from jax.experimental.pallas import tpu as pltpu
from jax.sharding import PartitionSpec as P

absent_score = -1e30
both_axes = ("seq", "grp")
all_axes = ("seq", "tp", "grp")
far = 1 << 20


def arrival_places(block_table, seq_index, group_index, slots, groups, ranges):
    rows, width = block_table.shape
    per_group, span = rows // groups, width // ranges
    own = lax.dynamic_slice(
        block_table, (group_index * per_group, seq_index * span), (per_group, span)
    )
    source = (own // slots)[None]
    place = lax.broadcasted_iota(jnp.int32, (1, per_group, span), 1) * span
    place = place + lax.broadcasted_iota(jnp.int32, (1, per_group, span), 2)
    here = source == jnp.arange(groups * ranges, dtype=jnp.int32)[:, None, None]
    return (
        jnp.min(jnp.where(here, place, far), axis=(1, 2)),
        jnp.max(jnp.where(here, place, -1), axis=(1, 2)),
    )


def code_at(codes, ranges, k, g, s):
    return codes[2 * g, k * ranges + s]


def gather_kernel(
    sizes, table_in, scales_in, pool, out, codes_out, lines_out,
    table, scales, codes, scale_lines, held, codes_s, load, store, side
):
    groups, ranges, slots, span = sizes
    rows = pool.shape[1]
    loads = []
    step = slots // 8
    for i in range(8):
        part = pl.ds(i * step, step)
        loads.append(pltpu.make_async_copy(pool.at[part], held.at[part], load.at[i]))
    small = [
        pltpu.make_async_copy(table_in, table, side.at[0]),
        pltpu.make_async_copy(scales_in, scales, side.at[1]),
    ]
    for copy in small + loads[:4]:
        copy.start()
    small[0].wait()
    source = lax.axis_index("seq") * groups + lax.axis_index("grp")
    entry = table[...]
    row = lax.broadcasted_iota(jnp.int32, entry.shape, 0)
    lane = lax.broadcasted_iota(jnp.int32, entry.shape, 1)
    code = ((row & 1) * span + (lane & (span - 1))) * slots + (entry & (slots - 1))
    code = code.astype(jnp.float32)
    mine = (entry >> (slots.bit_length() - 1)) == source
    found = jnp.full(entry.shape, float(far))
    for s in range(ranges):
        here = mine & ((lane >> (span.bit_length() - 1)) == s)
        for k, value in enumerate((code, -code)):
            least = jnp.min(jnp.where(here, value, float(far)), axis=1, keepdims=True)
            found = jnp.where(lane == k * ranges + s, least, found)
    found = jnp.minimum(found, pltpu.roll(found, entry.shape[0] - 1, 0))
    codes[...] = jnp.where(lane < ranges, found, -found).astype(jnp.int32)
    for copy in loads[4:]:
        copy.start()
    inner = pltpu.make_async_copy(codes, codes_s, side.at[2])
    inner.start()
    small[1].wait()
    scale_lines[...] = jnp.zeros(scale_lines.shape, jnp.float32)
    scale_lines[pl.ds(0, 2), pl.ds(0, slots)] = scales[...].astype(jnp.float32)
    lines = scale_lines[...]
    scale_lines[pl.ds(2, 1), :] = lines[0:1] + pltpu.roll(lines, slots, 1)[1:2]
    inner.wait()
    chosen = [
        code_at(codes_s, ranges, k, g, s) & (slots - 1)
        for s in range(ranges)
        for g in range(groups)
        for k in range(2)
    ]
    for copy in loads:
        copy.wait()
    stores = []
    for n, slot in enumerate(chosen):
        stores.append(
            pltpu.make_async_copy(
                held.at[slot], out.at[n // 2, pl.ds(n % 2 * rows, rows)], store.at[n]
            )
        )
        stores[-1].start()
    last = [
        pltpu.make_async_copy(codes, codes_out, side.at[3]),
        pltpu.make_async_copy(scale_lines, lines_out, side.at[4]),
    ]
    for copy in last:
        copy.start()
    for copy in stores + last:
        copy.wait()


def place_kernel(
    places_in, own_in, table_in, arrived, cache, scale_out, places, own, table, scale, held, load, store, side
):
    sources = arrived.shape[0]
    rows = cache.shape[1]
    step = sources // 8
    loads = []
    for i in range(8):
        part = pl.ds(i * step, step)
        loads.append(pltpu.make_async_copy(arrived.at[part], held.at[part], load.at[i]))
        loads[-1].start()
    small = [
        pltpu.make_async_copy(*pair, side.at[i])
        for i, pair in enumerate(((places_in, places), (own_in, own), (table_in, table)))
    ]
    for copy in small:
        copy.start()
    for copy in small:
        copy.wait()
    stores = []
    for d in range(sources):
        if d % step == 0:
            loads[d // step].wait()
        for k in range(2):
            stores.append(
                pltpu.make_async_copy(
                    held.at[d, pl.ds(k * rows, rows)], cache.at[places[k, d]], store.at[2 * d + k]
                )
            )
            stores[-1].start()
    members, _, span = scale.shape
    slots = table.shape[1] // 2
    row = lax.broadcasted_iota(jnp.int32, (8, 128), 0)
    lane = lax.broadcasted_iota(jnp.int32, (8, 128), 1)
    for b in range(members):
        lines = jnp.zeros((8, 128), jnp.float32)
        for j in range(span):
            source, slot = own[b, j] >> (slots.bit_length() - 1), own[b, j] & (slots - 1)
            pair = jnp.where(row == 0, table[source, slot], table[source, slots + slot])
            lines = jnp.where(lane == j, pair, lines)
        scale[b] = lines[:2, :span].astype(scale.dtype)
    for one in stores[:16]:
        one.wait()
    copy = pltpu.make_async_copy(scale, scale_out, side.at[3])
    copy.start()
    for one in stores[16:]:
        one.wait()
    copy.wait()


def stat_rows(peak, total, scale_line, half):
    row = lax.broadcasted_iota(jnp.int32, (half, 128), 0)
    lane = lax.broadcasted_iota(jnp.int32, (half, 128), 1)
    peak_row = jnp.sum(jnp.where(row == lane, peak, 0.0), axis=0, keepdims=True)
    total_row = jnp.sum(jnp.where(row == lane, total, 0.0), axis=0, keepdims=True)
    line = lax.broadcasted_iota(jnp.int32, (8, 128), 0)
    lines = jnp.where(line == 1, total_row, jnp.where(line == 2, scale_line, 0.0))
    return jnp.where(line == 0, peak_row, lines)


def as_column(line, half):
    row = lax.broadcasted_iota(jnp.int32, (half, 128), 0)
    lane = lax.broadcasted_iota(jnp.int32, (half, 128), 1)
    return jnp.sum(jnp.where(row == lane, line, 0.0), axis=1, keepdims=True)


def attend_kernel(
    sizes, codes, scales, lens, scale_lines, own_q, other_q, blocks, keep, give, held, peaks, totals, sem
):
    groups, ranges, slots, span, root_scale = sizes
    cores = 2
    chips = groups // cores
    bits, span_bits = slots.bit_length() - 1, span.bit_length() - 1
    size = blocks.shape[2]
    heads = own_q.shape[1] // 2
    group = lax.axis_index("grp")
    chip, core = group >> 1, group & 1
    order = [(flip, k) for flip in range(cores) for k in range(chips)]
    copies = []
    for i, (flip, k) in enumerate(order):
        g = cores * (chip ^ k) + (core ^ flip)
        for s in range(ranges):
            n = i * ranges + s
            copy = pltpu.make_async_copy(
                blocks.at[s * groups + g, pl.ds(0, 4 * size)], held.at[n], sem.at[n]
            )
            copy.start()
            copies.append(copy)
    line = lax.broadcasted_iota(jnp.int32, (2 * heads, size), 0)
    lane = lax.broadcasted_iota(jnp.int32, (2 * heads, size), 1)
    parts = []
    for copy in copies:
        copy.wait()
    for i, (flip, k) in enumerate(order):
        at = chip ^ k
        g = cores * at + (core ^ flip)
        query = (other_q if flip else own_q)[k]
        scored, lives, values = [], [], []
        for s in range(ranges):
            for kk in range(2):
                code = code_at(codes, ranges, kk, g, s)
                slot, place = code & (slots - 1), code >> bits
                member, column = place >> span_bits, place & (span - 1)
                limit = lens[2 * g + member] - (s * span + column) * size
                keys = held[i * ranges + s, pl.ds(2 * kk * size, size)]
                score = lax.dot_general(
                    query, keys, (((1,), (1,)), ((), ())), preferred_element_type=jnp.float32
                )
                low = member * heads
                live = (line >= low) & (line < low + heads) & (lane < limit)
                scored.append(
                    jnp.where(live, score * scales[0, slot] * root_scale, absent_score)
                )
                lives.append(live)
                values.append(scales[1, slot])
        peak = functools.reduce(jnp.maximum, scored)
        peak = jnp.max(peak, axis=1, keepdims=True)
        parts.append((at, flip, peak, scored, lives, values))
    for i, (at, flip, peak, scored, lives, values) in enumerate(parts):
        total, summed = 0.0, 0.0
        for n, (score, live, value) in enumerate(zip(scored, lives, values)):
            weight = jnp.where(live, jnp.exp(score - peak), 0.0)
            total = total + weight
            rows = held[i * ranges + n // 2, pl.ds((2 * (n % 2) + 1) * size, size)]
            summed = summed + jnp.dot(
                (weight * value).astype(jnp.bfloat16), rows, preferred_element_type=jnp.float32
            )
        total = jnp.sum(total, axis=1, keepdims=True)
        to = pl.ds(pl.multiple_of(at * 2 * heads, 2 * heads), 2 * heads)
        (give if flip else keep)[to, :] = summed
        peaks[flip, to, :] = jnp.broadcast_to(peak, (2 * heads, 128))
        totals[flip, to, :] = jnp.broadcast_to(total, (2 * heads, 128))
    half = chips * 2 * heads
    for flip, out in enumerate((keep, give)):
        out[pl.ds(half, 8), :] = stat_rows(
            peaks[flip], totals[flip], scale_lines[pl.ds(2, 1), :], half
        )


def in_three(value):
    parts = []
    for _ in range(3):
        part = value.astype(jnp.bfloat16)
        parts.append(part)
        value = value - part.astype(jnp.float32)
    return parts


def stats_of(part, half):
    tile = part[pl.ds(half, part.shape[0] - half), :].astype(jnp.float32)
    if part.dtype == jnp.float32:
        return tile[0:1], tile[1:2], [tile[2:3]]
    return (
        tile[2:3] + tile[1:2] + tile[0:1],
        tile[5:6] + tile[4:5] + tile[3:4],
        [tile[i : i + 1] for i in range(6, 14)],
    )


def merged(half, *parts):
    stats = [stats_of(part, half) for part in parts]
    peak = functools.reduce(jnp.maximum, [own_peak for own_peak, *_ in stats])
    total, summed = 0.0, 0.0
    for part, (own_peak, own_total, _) in zip(parts, stats):
        factor = jnp.exp(own_peak - peak)
        total = total + own_total * factor
        summed = summed + part[pl.ds(0, half), :].astype(jnp.float32) * as_column(factor, half)
    return peak, total, summed, [scales for *_, scales in stats]


def merge_kernel(*refs):
    *parts, out = refs
    half = out.shape[0] - 16
    peak, total, summed, scales = merged(half, *parts)
    out[pl.ds(0, half), :] = summed.astype(out.dtype)
    line = lax.broadcasted_iota(jnp.int32, (16, 128), 0)
    tile = jnp.zeros((16, 128), jnp.float32)
    for i, part in enumerate(in_three(peak) + in_three(total)):
        tile = jnp.where(line == i, part.astype(jnp.float32), tile)
    chip, core = lax.axis_index("grp") >> 1, lax.axis_index("grp") & 1
    for k, lines in enumerate(scales):
        if len(lines) == 1:
            tile = jnp.where(line == 6 + (core ^ k), lines[0], tile)
        else:
            for i in range(2):
                tile = jnp.where(line == 6 + 2 * (chip ^ k) + i, lines[i], tile)
    out[pl.ds(half, 16), :] = tile.astype(out.dtype)


def finish_kernel(*refs):
    *parts, out, table = refs
    half = out.shape[0]
    _, total, summed, scales = merged(half, *parts)
    out[...] = summed / as_column(total, half)
    here = lax.axis_index("seq")
    for k, lines in enumerate(scales):
        to = pl.ds(pl.multiple_of((here ^ k) * len(lines), len(lines)), len(lines))
        table[to, :] = jnp.concatenate(lines, axis=0)


def project_kernel(own, other, weight, keep, give, slots):
    size = own.shape[1]
    heads = weight.shape[0] // size
    lines = own.shape[0] // heads
    summed = 0.0
    for k in range(heads):
        rows = jnp.concatenate(
            [ref[pl.ds(k, lines, stride=heads), :] for ref in (own, other)], axis=0
        )
        summed = summed + jnp.dot(
            rows.astype(jnp.bfloat16),
            weight[pl.ds(k * size, size), :],
            preferred_element_type=jnp.float32,
        )
    core = lax.axis_index("grp") & 1
    here = lax.axis_index("tp")
    count = keep.shape[0]
    for flip in range(2):
        for at in range(lines // 2):
            j = (2 * at + (core ^ flip)) ^ here
            first = flip * lines + 2 * at
            pair = j >> 1
            given = (j & 1) ^ jnp.where(pair == 2, 1, 0)
            slots[pair + count * given] = summed[first : first + 2]
    keep[...] = slots[pl.ds(0, count)]
    give[...] = slots[pl.ds(count, count)]


def split_kernel(keep, came, *outs):
    for i, out in enumerate(outs):
        out[...] = keep[i] + came[i]


def add_kernel(*refs):
    *terms, out = refs
    total = terms[0][...]
    for term in terms[1:]:
        total = total + term[...]
    out[...] = total.astype(out.dtype)


tight = pltpu.CompilerParams(vmem_limit_bytes=4 * 1024 * 1024)
wide = pltpu.CompilerParams(vmem_limit_bytes=60 * 1024 * 1024)
middle = pltpu.CompilerParams(vmem_limit_bytes=50 * 1024 * 1024)
smem = pl.BlockSpec(memory_space=pltpu.SMEM)
vmem = pl.BlockSpec(memory_space=pltpu.VMEM)
hbm = pl.BlockSpec(memory_space=pltpu.HBM)


def flipped(array, y=0, z=0, x=0, core=0):
    tps, grps = lax.axis_size("tp"), lax.axis_size("grp")
    pairs = []
    for i in range(lax.axis_size("seq") * tps * grps):
        a, b, c = i // (tps * grps), i // grps % tps, i % grps
        pairs.append((i, ((a ^ y) * tps + (b ^ z)) * grps + (c ^ (2 * x + core))))
    return lax.ppermute(array, all_axes, pairs)


def merge(parts, kernel, out_shape):
    return pl.pallas_call(
        kernel,
        out_shape=out_shape,
        in_specs=[vmem] * len(parts),
        out_specs=jax.tree.map(lambda _: vmem, out_shape),
        compiler_params=tight,
    )(*parts)


def per_device(queries, cache_pool, block_scale, block_table, lengths, output_weight):
    seq_count = lax.axis_size("seq")
    group_count = lax.axis_size("grp")
    tp_count = lax.axis_size("tp")
    sources = seq_count * group_count
    chips = group_count // 2
    pool_slots = cache_pool.shape[0]
    key_heads = cache_pool.shape[1]
    block_size = cache_pool.shape[3]
    head_size = cache_pool.shape[4]
    batch_rows, table_width = block_table.shape
    per_group = batch_rows // group_count
    share_blocks = table_width // seq_count
    heads_here = queries.shape[1]
    out_width = output_weight.shape[1]
    root_scale = 1.0 / math.sqrt(head_size)
    rows = 2 * block_size

    flat_queries = queries.reshape(per_group * heads_here, head_size)
    abroad = flipped(flat_queries, z=1)
    outgoing, codes, scale_lines = pl.pallas_call(
        functools.partial(gather_kernel, (group_count, seq_count, pool_slots, share_blocks)),
        out_shape=(
            jax.ShapeDtypeStruct((sources, 2 * rows, head_size), cache_pool.dtype),
            jax.ShapeDtypeStruct(block_table.shape, jnp.int32),
            jax.ShapeDtypeStruct((8, 128), jnp.float32),
        ),
        in_specs=[hbm, hbm, hbm],
        out_specs=(hbm, hbm, hbm),
        scratch_shapes=[
            pltpu.VMEM(block_table.shape, jnp.int32),
            pltpu.VMEM((2, pool_slots), block_scale.dtype),
            pltpu.VMEM(block_table.shape, jnp.int32),
            pltpu.VMEM((8, 128), jnp.float32),
            pltpu.VMEM((pool_slots, rows, head_size), cache_pool.dtype),
            pltpu.SMEM(block_table.shape, jnp.int32),
            pltpu.SemaphoreType.DMA((8,)),
            pltpu.SemaphoreType.DMA((2 * sources,)),
            pltpu.SemaphoreType.DMA((5,)),
        ],
        compiler_params=wide,
    )(
        block_table,
        block_scale.reshape(pool_slots, 2).T,
        cache_pool.reshape(pool_slots, rows, head_size),
    )
    outgoing, abroad = lax.optimization_barrier((outgoing, abroad))
    arrived = lax.all_to_all(outgoing, both_axes, split_axis=0, concat_axis=0, tiled=True)

    own_q = jnp.stack(
        [flat_queries] + [flipped(abroad, x=k, z=1) for k in range(1, chips)]
    )
    other_q = flipped(own_q, core=1)

    half = chips * per_group * heads_here
    line_shape = jax.ShapeDtypeStruct((half + 8, head_size), jnp.float32)
    keep, give = pl.pallas_call(
        functools.partial(
            attend_kernel, (group_count, seq_count, pool_slots, share_blocks, root_scale)
        ),
        out_shape=(line_shape, line_shape),
        in_specs=[smem, smem, smem, vmem, vmem, vmem, hbm],
        out_specs=(vmem, vmem),
        scratch_shapes=[
            pltpu.VMEM((sources, 2 * rows, head_size), cache_pool.dtype),
            pltpu.VMEM((2, half, 128), jnp.float32),
            pltpu.VMEM((2, half, 128), jnp.float32),
            pltpu.SemaphoreType.DMA((sources,)),
        ],
        compiler_params=middle,
    )(codes, scale_lines, lengths, scale_lines, own_q, other_q, outgoing)
    message = jax.ShapeDtypeStruct((half + 16, head_size), jnp.bfloat16)
    lines = merge([keep, flipped(give, core=1)], merge_kernel, message)
    lines = merge([flipped(lines, z=1, x=k) for k in range(chips)], merge_kernel, message)
    lines, scale_table = merge(
        [flipped(lines, z=1, y=k) for k in range(seq_count)],
        finish_kernel,
        (
            jax.ShapeDtypeStruct((half, head_size), jnp.float32),
            jax.ShapeDtypeStruct((sources, 128), jnp.float32),
        ),
    )
    places = jnp.stack(
        arrival_places(
            block_table,
            lax.axis_index("seq"),
            lax.axis_index("grp"),
            pool_slots,
            group_count,
            seq_count,
        )
    )
    own_entries = lax.dynamic_slice(
        block_table,
        (lax.axis_index("grp") * per_group, lax.axis_index("seq") * share_blocks),
        (per_group, share_blocks),
    )
    other_lines, places, own_entries = lax.optimization_barrier(
        (flipped(lines, core=1), places, own_entries)
    )
    pair_shape = jax.ShapeDtypeStruct((tp_count // 2, per_group, out_width), jnp.float32)
    keep, give = pl.pallas_call(
        project_kernel,
        out_shape=(pair_shape, pair_shape),
        in_specs=[vmem, vmem, vmem],
        out_specs=(vmem, vmem),
        scratch_shapes=[pltpu.VMEM((tp_count, per_group, out_width), jnp.float32)],
        compiler_params=tight,
    )(lines, other_lines, output_weight)
    share = jax.ShapeDtypeStruct((per_group, out_width), jnp.float32)
    shares = pl.pallas_call(
        split_kernel,
        out_shape=(share,) * (tp_count // 2),
        in_specs=[vmem, vmem],
        out_specs=(vmem,) * (tp_count // 2),
        compiler_params=tight,
    )(keep, flipped(give, z=1))
    terms = [shares[0]] + [flipped(shares[i], z=z) for i, z in ((1, 2), (2, 5), (3, 6))]
    placed, scales = pl.pallas_call(
        place_kernel,
        out_shape=(
            jax.ShapeDtypeStruct((pool_slots, rows, head_size), cache_pool.dtype),
            jax.ShapeDtypeStruct((per_group, 2, share_blocks), block_scale.dtype),
        ),
        in_specs=[vmem, vmem, vmem, hbm],
        out_specs=(hbm, hbm),
        scratch_shapes=[
            pltpu.SMEM((2, sources), jnp.int32),
            pltpu.SMEM((per_group, share_blocks), jnp.int32),
            pltpu.SMEM((sources, 128), jnp.float32),
            pltpu.VMEM((per_group, 2, share_blocks), block_scale.dtype),
            pltpu.VMEM((sources, 2 * rows, head_size), cache_pool.dtype),
            pltpu.SemaphoreType.DMA((8,)),
            pltpu.SemaphoreType.DMA((2 * sources,)),
            pltpu.SemaphoreType.DMA((4,)),
        ],
        compiler_params=middle,
    )(places, own_entries, scale_table, arrived)
    terms, scales = lax.optimization_barrier((terms, scales))
    summed = pl.pallas_call(
        add_kernel,
        out_shape=jax.ShapeDtypeStruct((per_group, out_width), jnp.bfloat16),
        in_specs=[vmem] * len(terms),
        out_specs=vmem,
        compiler_params=tight,
    )(*terms)
    decode_cache = placed.reshape(
        per_group, share_blocks, key_heads, 2, block_size, head_size
    )
    decode_scale = scales.transpose(0, 2, 1).reshape(per_group, share_blocks, key_heads, 2)
    return (summed, decode_cache, decode_scale)


def solution(mesh):
    placed = (
        P("grp", "tp", None),
        P(("seq", "grp"), "tp", None, None, None),
        P(("seq", "grp"), "tp", None),
        P(),
        P(),
        P("tp", ("seq", "grp")),
    )
    return jax.shard_map(
        per_device,
        mesh=mesh,
        in_specs=placed,
        out_specs=(
            P("tp", ("seq", "grp")),
            P("grp", "seq", "tp", None, None, None),
            P("grp", "seq", "tp", None),
        ),
        check_vma=False,
    )
```

```python
import functools
import math

import jax
import jax.numpy as jnp
from jax import lax
from jax.experimental import pallas as pl
from jax.experimental.pallas import tpu as pltpu
from jax.sharding import PartitionSpec as P

absent_score = -1e30
both_axes = ("seq", "grp")
all_axes = ("seq", "tp", "grp")
far = 1 << 20


def rank_of(s, g, groups, ranges):
    return groups * ranges - 1 - (s * groups + g)


def ranked(groups, ranges):
    pairs = [(s, g) for s in range(ranges) for g in range(groups)]
    return sorted(pairs, key=lambda pair: rank_of(*pair, groups, ranges))


def code_at(codes, ranges, k, g, s):
    return codes[2 * g, k * ranges + s]


def gather_kernel(
    sizes, table_in, scales_in, pool, out, codes_out, lines_out,
    table, scales, codes, scale_lines, held, codes_s, load, store, side
):
    groups, ranges, slots, span = sizes
    rows = pool.shape[1]
    loads = []
    step = slots // 8
    for i in range(8):
        part = pl.ds(i * step, step)
        loads.append(pltpu.make_async_copy(pool.at[part], held.at[part], load.at[i]))
    small = [
        pltpu.make_async_copy(table_in, table, side.at[0]),
        pltpu.make_async_copy(scales_in, scales, side.at[1]),
    ]
    for copy in small + loads:
        copy.start()
    small[0].wait()
    source = lax.axis_index("seq") * groups + lax.axis_index("grp")
    entry = table[...]
    row = lax.broadcasted_iota(jnp.int32, entry.shape, 0)
    lane = lax.broadcasted_iota(jnp.int32, entry.shape, 1)
    code = ((row & 1) * span + (lane & (span - 1))) * slots + (entry & (slots - 1))
    code = code.astype(jnp.float32)
    mine = (entry >> (slots.bit_length() - 1)) == source
    found = jnp.full(entry.shape, float(far))
    for s in range(ranges):
        here = mine & ((lane >> (span.bit_length() - 1)) == s)
        for k, value in enumerate((code, -code)):
            least = jnp.min(jnp.where(here, value, float(far)), axis=1, keepdims=True)
            found = jnp.where(lane == k * ranges + s, least, found)
    found = jnp.minimum(found, pltpu.roll(found, entry.shape[0] - 1, 0))
    codes[...] = jnp.where(lane < ranges, found, -found).astype(jnp.int32)
    small[1].wait()
    scale_lines[...] = jnp.zeros(scale_lines.shape, jnp.float32)
    scale_lines[pl.ds(0, 2), pl.ds(0, slots)] = scales[...].astype(jnp.float32)
    lines = scale_lines[...]
    scale_lines[pl.ds(2, 1), :] = lines[0:1] + pltpu.roll(lines, slots, 1)[1:2]
    inner = pltpu.make_async_copy(codes, codes_s, side.at[2])
    inner.start()
    inner.wait()
    chosen = [
        code_at(codes_s, ranges, k, g, s) & (slots - 1)
        for s, g in ranked(groups, ranges)
        for k in range(2)
    ]
    for copy in loads:
        copy.wait()
    stores = []
    for n, slot in enumerate(chosen):
        stores.append(
            pltpu.make_async_copy(
                held.at[slot], out.at[n // 2, pl.ds(n % 2 * rows, rows)], store.at[n]
            )
        )
        stores[-1].start()
    last = [
        pltpu.make_async_copy(codes, codes_out, side.at[3]),
        pltpu.make_async_copy(scale_lines, lines_out, side.at[4]),
    ]
    for copy in last:
        copy.start()
    for copy in stores + last:
        copy.wait()


def place_kernel(
    ranges, entries_in, table_in, arrived, cache, scale_out, entries, places, seen, table, scale, held, load, store, side
):
    sources = arrived.shape[0]
    rows = cache.shape[1]
    step = sources // 8
    loads = []
    for i in range(8):
        part = pl.ds(i * step, step)
        loads.append(pltpu.make_async_copy(arrived.at[part], held.at[part], load.at[i]))
        loads[-1].start()
    small = [
        pltpu.make_async_copy(*pair, side.at[i])
        for i, pair in enumerate(((entries_in, entries), (table_in, table)))
    ]
    for copy in small:
        copy.start()
    for d in range(sources):
        seen[d] = 0
    members, _, span = scale.shape
    slots = table.shape[1] // 2
    first_row = lax.axis_index("grp") * members
    first_column = lax.axis_index("seq") * span
    small[0].wait()
    for b in range(members):
        for j in range(span):
            source = entries[first_row + b, first_column + j] >> (slots.bit_length() - 1)
            count = seen[source] & 1
            seen[source] = count + 1
            places[count, source] = b * span + j
    stores = []
    for d, (s, g) in enumerate(ranked(sources // ranges, ranges)):
        source = s * (sources // ranges) + g
        if d % step == 0:
            loads[d // step].wait()
        for k in range(2):
            stores.append(
                pltpu.make_async_copy(
                    held.at[d, pl.ds(k * rows, rows)], cache.at[places[k, source]], store.at[2 * d + k]
                )
            )
            stores[-1].start()
    small[1].wait()
    row = lax.broadcasted_iota(jnp.int32, (8, 128), 0)
    lane = lax.broadcasted_iota(jnp.int32, (8, 128), 1)
    for b in range(members):
        lines = jnp.zeros((8, 128), jnp.float32)
        for j in range(span):
            entry = entries[first_row + b, first_column + j]
            source, slot = entry >> (slots.bit_length() - 1), entry & (slots - 1)
            pair = jnp.where(row == 0, table[source, slot], table[source, slots + slot])
            lines = jnp.where(lane == j, pair, lines)
        scale[b] = lines[:2, :span].astype(scale.dtype)
    for one in stores[:16]:
        one.wait()
    copy = pltpu.make_async_copy(scale, scale_out, side.at[3])
    copy.start()
    for one in stores[16:]:
        one.wait()
    copy.wait()


def stat_rows(peak, total, scale_line, half):
    row = lax.broadcasted_iota(jnp.int32, (half, 128), 0)
    lane = lax.broadcasted_iota(jnp.int32, (half, 128), 1)
    peak_row = jnp.sum(jnp.where(row == lane, peak, 0.0), axis=0, keepdims=True)
    total_row = jnp.sum(jnp.where(row == lane, total, 0.0), axis=0, keepdims=True)
    line = lax.broadcasted_iota(jnp.int32, (8, 128), 0)
    lines = jnp.where(line == 1, total_row, jnp.where(line == 2, scale_line, 0.0))
    return jnp.where(line == 0, peak_row, lines)


def as_column(line, half):
    row = lax.broadcasted_iota(jnp.int32, (half, 128), 0)
    lane = lax.broadcasted_iota(jnp.int32, (half, 128), 1)
    return jnp.sum(jnp.where(row == lane, line, 0.0), axis=1, keepdims=True)


def attend_kernel(
    sizes, codes, scales, lens, scale_lines, own_q, other_q, blocks, keep, give, held, peaks, totals, sem
):
    groups, ranges, slots, span, root_scale = sizes
    cores = 2
    chips = groups // cores
    bits, span_bits = slots.bit_length() - 1, span.bit_length() - 1
    size = blocks.shape[2]
    heads = own_q.shape[1] // 2
    group = lax.axis_index("grp")
    chip, core = group >> 1, group & 1
    order = [(flip, k) for flip in range(cores) for k in range(chips)]
    copies = []
    for i, (flip, k) in enumerate(order):
        g = cores * (chip ^ k) + (core ^ flip)
        for s in range(ranges):
            n = i * ranges + s
            copy = pltpu.make_async_copy(
                blocks.at[rank_of(s, g, groups, ranges), pl.ds(0, 4 * size)], held.at[n], sem.at[n]
            )
            copy.start()
            copies.append(copy)
    line = lax.broadcasted_iota(jnp.int32, (2 * heads, size), 0)
    lane = lax.broadcasted_iota(jnp.int32, (2 * heads, size), 1)
    parts = []
    for copy in copies:
        copy.wait()
    for i, (flip, k) in enumerate(order):
        at = chip ^ k
        g = cores * at + (core ^ flip)
        query = (other_q if flip else own_q)[k]
        scored, lives, values = [], [], []
        for s in range(ranges):
            for kk in range(2):
                code = code_at(codes, ranges, kk, g, s)
                slot, place = code & (slots - 1), code >> bits
                member, column = place >> span_bits, place & (span - 1)
                limit = lens[2 * g + member] - (s * span + column) * size
                keys = held[i * ranges + s, pl.ds(2 * kk * size, size)]
                score = lax.dot_general(
                    query, keys, (((1,), (1,)), ((), ())), preferred_element_type=jnp.float32
                )
                low = member * heads
                live = (line >= low) & (line < low + heads) & (lane < limit)
                scored.append(
                    jnp.where(live, score * scales[0, slot] * root_scale, absent_score)
                )
                lives.append(live)
                values.append(scales[1, slot])
        peak = functools.reduce(jnp.maximum, scored)
        peak = jnp.max(peak, axis=1, keepdims=True)
        parts.append((at, flip, peak, scored, lives, values))
    for i, (at, flip, peak, scored, lives, values) in enumerate(parts):
        total, summed = 0.0, 0.0
        for n, (score, live, value) in enumerate(zip(scored, lives, values)):
            weight = jnp.where(live, jnp.exp(score - peak), 0.0)
            total = total + weight
            rows = held[i * ranges + n // 2, pl.ds((2 * (n % 2) + 1) * size, size)]
            summed = summed + jnp.dot(
                (weight * value).astype(jnp.bfloat16), rows, preferred_element_type=jnp.float32
            )
        total = jnp.sum(total, axis=1, keepdims=True)
        to = pl.ds(pl.multiple_of(at * 2 * heads, 2 * heads), 2 * heads)
        (give if flip else keep)[to, :] = summed
        peaks[flip, to, :] = jnp.broadcast_to(peak, (2 * heads, 128))
        totals[flip, to, :] = jnp.broadcast_to(total, (2 * heads, 128))
    half = chips * 2 * heads
    for flip, out in enumerate((keep, give)):
        out[pl.ds(half, 8), :] = stat_rows(
            peaks[flip], totals[flip], scale_lines[pl.ds(2, 1), :], half
        )


def in_three(value):
    parts = []
    for _ in range(3):
        part = value.astype(jnp.bfloat16)
        parts.append(part)
        value = value - part.astype(jnp.float32)
    return parts


def stats_of(part, half):
    tile = part[pl.ds(half, part.shape[0] - half), :].astype(jnp.float32)
    if part.dtype == jnp.float32:
        return tile[0:1], tile[1:2], [tile[2:3]]
    return (
        tile[2:3] + tile[1:2] + tile[0:1],
        tile[5:6] + tile[4:5] + tile[3:4],
        [tile[i : i + 1] for i in range(6, 14)],
    )


def merged(half, *parts):
    stats = [stats_of(part, half) for part in parts]
    peak = functools.reduce(jnp.maximum, [own_peak for own_peak, *_ in stats])
    total, summed = 0.0, 0.0
    for part, (own_peak, own_total, _) in zip(parts, stats):
        factor = jnp.exp(own_peak - peak)
        total = total + own_total * factor
        summed = summed + part[pl.ds(0, half), :].astype(jnp.float32) * as_column(factor, half)
    return peak, total, summed, [scales for *_, scales in stats]


def merge_kernel(*refs):
    *parts, out = refs
    half = out.shape[0] - 16
    peak, total, summed, scales = merged(half, *parts)
    out[pl.ds(0, half), :] = summed.astype(out.dtype)
    line = lax.broadcasted_iota(jnp.int32, (16, 128), 0)
    tile = jnp.zeros((16, 128), jnp.float32)
    for i, part in enumerate(in_three(peak) + in_three(total)):
        tile = jnp.where(line == i, part.astype(jnp.float32), tile)
    chip, core = lax.axis_index("grp") >> 1, lax.axis_index("grp") & 1
    for k, lines in enumerate(scales):
        if len(lines) == 1:
            tile = jnp.where(line == 6 + (core ^ k), lines[0], tile)
        else:
            for i in range(2):
                tile = jnp.where(line == 6 + 2 * (chip ^ k) + i, lines[i], tile)
    out[pl.ds(half, 16), :] = tile.astype(out.dtype)


def finish_kernel(*refs):
    *parts, out, table = refs
    half = out.shape[0]
    _, total, summed, scales = merged(half, *parts)
    out[...] = summed / as_column(total, half)
    here = lax.axis_index("seq")
    for k, lines in enumerate(scales):
        to = pl.ds(pl.multiple_of((here ^ k) * len(lines), len(lines)), len(lines))
        table[to, :] = jnp.concatenate(lines, axis=0)


def project_kernel(own, other, weight, keep, give, slots):
    size = own.shape[1]
    heads = weight.shape[0] // size
    lines = own.shape[0] // heads
    summed = 0.0
    for k in range(heads):
        rows = jnp.concatenate(
            [ref[pl.ds(k, lines, stride=heads), :] for ref in (own, other)], axis=0
        )
        summed = summed + jnp.dot(
            rows.astype(jnp.bfloat16),
            weight[pl.ds(k * size, size), :],
            preferred_element_type=jnp.float32,
        )
    core = lax.axis_index("grp") & 1
    here = lax.axis_index("tp")
    count = keep.shape[0]
    for flip in range(2):
        for at in range(lines // 2):
            j = (2 * at + (core ^ flip)) ^ here
            first = flip * lines + 2 * at
            pair = j >> 1
            given = (j & 1) ^ jnp.where(pair == 2, 1, 0)
            slots[pair + count * given] = summed[first : first + 2]
    keep[...] = slots[pl.ds(0, count)]
    give[...] = slots[pl.ds(count, count)]


def split_kernel(keep, came, *outs):
    for i, out in enumerate(outs):
        out[...] = keep[i] + came[i]


def add_kernel(*refs):
    *terms, out = refs
    total = terms[0][...]
    for term in terms[1:]:
        total = total + term[...]
    out[...] = total.astype(out.dtype)


tight = pltpu.CompilerParams(vmem_limit_bytes=4 * 1024 * 1024)
wide = pltpu.CompilerParams(vmem_limit_bytes=60 * 1024 * 1024)
middle = pltpu.CompilerParams(vmem_limit_bytes=50 * 1024 * 1024)
smem = pl.BlockSpec(memory_space=pltpu.SMEM)
vmem = pl.BlockSpec(memory_space=pltpu.VMEM)
hbm = pl.BlockSpec(memory_space=pltpu.HBM)


def flipped(array, y=0, z=0, x=0, core=0):
    tps, grps = lax.axis_size("tp"), lax.axis_size("grp")
    pairs = []
    for i in range(lax.axis_size("seq") * tps * grps):
        a, b, c = i // (tps * grps), i // grps % tps, i % grps
        pairs.append((i, ((a ^ y) * tps + (b ^ z)) * grps + (c ^ (2 * x + core))))
    return lax.ppermute(array, all_axes, pairs)


def merge(parts, kernel, out_shape):
    return pl.pallas_call(
        kernel,
        out_shape=out_shape,
        in_specs=[vmem] * len(parts),
        out_specs=jax.tree.map(lambda _: vmem, out_shape),
        compiler_params=tight,
    )(*parts)


def per_device(queries, cache_pool, block_scale, block_table, lengths, output_weight):
    seq_count = lax.axis_size("seq")
    group_count = lax.axis_size("grp")
    tp_count = lax.axis_size("tp")
    sources = seq_count * group_count
    chips = group_count // 2
    pool_slots = cache_pool.shape[0]
    key_heads = cache_pool.shape[1]
    block_size = cache_pool.shape[3]
    head_size = cache_pool.shape[4]
    batch_rows, table_width = block_table.shape
    per_group = batch_rows // group_count
    share_blocks = table_width // seq_count
    heads_here = queries.shape[1]
    out_width = output_weight.shape[1]
    root_scale = 1.0 / math.sqrt(head_size)
    rows = 2 * block_size

    flat_queries = queries.reshape(per_group * heads_here, head_size)
    abroad = flipped(flat_queries, z=1)
    outgoing, codes, scale_lines = pl.pallas_call(
        functools.partial(gather_kernel, (group_count, seq_count, pool_slots, share_blocks)),
        out_shape=(
            jax.ShapeDtypeStruct((sources, 2 * rows, head_size), cache_pool.dtype),
            jax.ShapeDtypeStruct(block_table.shape, jnp.int32),
            jax.ShapeDtypeStruct((8, 128), jnp.float32),
        ),
        in_specs=[hbm, hbm, hbm],
        out_specs=(hbm, hbm, hbm),
        scratch_shapes=[
            pltpu.VMEM(block_table.shape, jnp.int32),
            pltpu.VMEM((2, pool_slots), block_scale.dtype),
            pltpu.VMEM(block_table.shape, jnp.int32),
            pltpu.VMEM((8, 128), jnp.float32),
            pltpu.VMEM((pool_slots, rows, head_size), cache_pool.dtype),
            pltpu.SMEM(block_table.shape, jnp.int32),
            pltpu.SemaphoreType.DMA((8,)),
            pltpu.SemaphoreType.DMA((2 * sources,)),
            pltpu.SemaphoreType.DMA((5,)),
        ],
        compiler_params=wide,
    )(
        block_table,
        block_scale.reshape(pool_slots, 2).T,
        cache_pool.reshape(pool_slots, rows, head_size),
    )
    outgoing, abroad = lax.optimization_barrier((outgoing, abroad))
    order = [s * group_count + g for s, g in ranked(group_count, seq_count)]
    arrived = lax.all_to_all(
        outgoing, both_axes, split_axis=0, concat_axis=0, axis_index_groups=[order], tiled=True
    )

    own_q = jnp.stack(
        [flat_queries] + [flipped(abroad, x=k, z=1) for k in range(1, chips)]
    )
    other_q = flipped(own_q, core=1)

    half = chips * per_group * heads_here
    line_shape = jax.ShapeDtypeStruct((half + 8, head_size), jnp.float32)
    keep, give = pl.pallas_call(
        functools.partial(
            attend_kernel, (group_count, seq_count, pool_slots, share_blocks, root_scale)
        ),
        out_shape=(line_shape, line_shape),
        in_specs=[smem, smem, smem, vmem, vmem, vmem, hbm],
        out_specs=(vmem, vmem),
        scratch_shapes=[
            pltpu.VMEM((sources, 2 * rows, head_size), cache_pool.dtype),
            pltpu.VMEM((2, half, 128), jnp.float32),
            pltpu.VMEM((2, half, 128), jnp.float32),
            pltpu.SemaphoreType.DMA((sources,)),
        ],
        compiler_params=middle,
    )(codes, scale_lines, lengths, scale_lines, own_q, other_q, outgoing)
    message = jax.ShapeDtypeStruct((half + 16, head_size), jnp.bfloat16)
    lines = merge([keep, flipped(give, core=1)], merge_kernel, message)
    lines = merge([flipped(lines, z=1, x=k) for k in range(chips)], merge_kernel, message)
    lines, scale_table = merge(
        [flipped(lines, z=1, y=k) for k in range(seq_count)],
        finish_kernel,
        (
            jax.ShapeDtypeStruct((half, head_size), jnp.float32),
            jax.ShapeDtypeStruct((sources, 128), jnp.float32),
        ),
    )
    other_lines = flipped(lines, core=1)
    pair_shape = jax.ShapeDtypeStruct((tp_count // 2, per_group, out_width), jnp.float32)
    keep, give = pl.pallas_call(
        project_kernel,
        out_shape=(pair_shape, pair_shape),
        in_specs=[vmem, vmem, vmem],
        out_specs=(vmem, vmem),
        scratch_shapes=[pltpu.VMEM((tp_count, per_group, out_width), jnp.float32)],
        compiler_params=tight,
    )(lines, other_lines, output_weight)
    share = jax.ShapeDtypeStruct((per_group, out_width), jnp.float32)
    shares = pl.pallas_call(
        split_kernel,
        out_shape=(share,) * (tp_count // 2),
        in_specs=[vmem, vmem],
        out_specs=(vmem,) * (tp_count // 2),
        compiler_params=tight,
    )(keep, flipped(give, z=1))
    terms = [shares[0]] + [flipped(shares[i], z=z) for i, z in ((1, 2), (2, 5), (3, 6))]
    placed, scales = pl.pallas_call(
        functools.partial(place_kernel, seq_count),
        out_shape=(
            jax.ShapeDtypeStruct((pool_slots, rows, head_size), cache_pool.dtype),
            jax.ShapeDtypeStruct((per_group, 2, share_blocks), block_scale.dtype),
        ),
        in_specs=[hbm, vmem, hbm],
        out_specs=(hbm, hbm),
        scratch_shapes=[
            pltpu.SMEM(block_table.shape, jnp.int32),
            pltpu.SMEM((2, sources), jnp.int32),
            pltpu.SMEM((sources,), jnp.int32),
            pltpu.SMEM((sources, 128), jnp.float32),
            pltpu.VMEM((per_group, 2, share_blocks), block_scale.dtype),
            pltpu.VMEM((sources, 2 * rows, head_size), cache_pool.dtype),
            pltpu.SemaphoreType.DMA((8,)),
            pltpu.SemaphoreType.DMA((2 * sources,)),
            pltpu.SemaphoreType.DMA((4,)),
        ],
        compiler_params=middle,
    )(block_table, scale_table, arrived)
    terms, scales = lax.optimization_barrier((terms, scales))
    summed = pl.pallas_call(
        add_kernel,
        out_shape=jax.ShapeDtypeStruct((per_group, out_width), jnp.bfloat16),
        in_specs=[vmem] * len(terms),
        out_specs=vmem,
        compiler_params=tight,
    )(*terms)
    decode_cache = placed.reshape(
        per_group, share_blocks, key_heads, 2, block_size, head_size
    )
    decode_scale = scales.transpose(0, 2, 1).reshape(per_group, share_blocks, key_heads, 2)
    return (summed, decode_cache, decode_scale)


def solution(mesh):
    placed = (
        P("grp", "tp", None),
        P(("seq", "grp"), "tp", None, None, None),
        P(("seq", "grp"), "tp", None),
        P(),
        P(),
        P("tp", ("seq", "grp")),
    )
    return jax.shard_map(
        per_device,
        mesh=mesh,
        in_specs=placed,
        out_specs=(
            P("tp", ("seq", "grp")),
            P("grp", "seq", "tp", None, None, None),
            P("grp", "seq", "tp", None),
        ),
        check_vma=False,
    )
```

```python
import functools
import math

import jax
import jax.numpy as jnp
from jax import lax
from jax.experimental import pallas as pl
from jax.experimental.pallas import tpu as pltpu
from jax.sharding import PartitionSpec as P

absent_score = -1e30
both_axes = ("seq", "grp")
all_axes = ("seq", "tp", "grp")
far = 1 << 20


def rank_of(s, g, groups, ranges):
    return groups * ranges - 1 - (s * groups + g)


def ranked(groups, ranges):
    pairs = [(s, g) for s in range(ranges) for g in range(groups)]
    return sorted(pairs, key=lambda pair: rank_of(*pair, groups, ranges))


def code_at(codes, ranges, k, g, s):
    return codes[2 * g, k * ranges + s]


def gather_kernel(
    sizes, table_in, scales_in, pool, out, codes_out, lines_out,
    table, scales, codes, scale_lines, held, codes_s, load, store, side
):
    groups, ranges, slots, span = sizes
    rows = pool.shape[1]
    loads = []
    step = slots // 8
    for i in range(8):
        part = pl.ds(i * step, step)
        loads.append(pltpu.make_async_copy(pool.at[part], held.at[part], load.at[i]))
    small = [
        pltpu.make_async_copy(table_in, table, side.at[0]),
        pltpu.make_async_copy(scales_in, scales, side.at[1]),
    ]
    for copy in small + loads:
        copy.start()
    small[0].wait()
    source = lax.axis_index("seq") * groups + lax.axis_index("grp")
    entry = table[...]
    row = lax.broadcasted_iota(jnp.int32, entry.shape, 0)
    lane = lax.broadcasted_iota(jnp.int32, entry.shape, 1)
    code = ((row & 1) * span + (lane & (span - 1))) * slots + (entry & (slots - 1))
    code = code.astype(jnp.float32)
    mine = (entry >> (slots.bit_length() - 1)) == source
    found = jnp.full(entry.shape, float(far))
    for s in range(ranges):
        here = mine & ((lane >> (span.bit_length() - 1)) == s)
        for k, value in enumerate((code, -code)):
            least = jnp.min(jnp.where(here, value, float(far)), axis=1, keepdims=True)
            found = jnp.where(lane == k * ranges + s, least, found)
    found = jnp.minimum(found, pltpu.roll(found, entry.shape[0] - 1, 0))
    codes[...] = jnp.where(lane < ranges, found, -found).astype(jnp.int32)
    small[1].wait()
    scale_lines[...] = jnp.zeros(scale_lines.shape, jnp.float32)
    scale_lines[pl.ds(0, 2), pl.ds(0, slots)] = scales[...].astype(jnp.float32)
    lines = scale_lines[...]
    scale_lines[pl.ds(2, 1), :] = lines[0:1] + pltpu.roll(lines, slots, 1)[1:2]
    inner = pltpu.make_async_copy(codes, codes_s, side.at[2])
    inner.start()
    inner.wait()
    chosen = [
        code_at(codes_s, ranges, k, g, s) & (slots - 1)
        for s, g in ranked(groups, ranges)
        for k in range(2)
    ]
    for copy in loads:
        copy.wait()
    stores = []
    for n, slot in enumerate(chosen):
        stores.append(
            pltpu.make_async_copy(
                held.at[slot], out.at[n // 2, pl.ds(n % 2 * rows, rows)], store.at[n]
            )
        )
        stores[-1].start()
    last = [
        pltpu.make_async_copy(codes, codes_out, side.at[3]),
        pltpu.make_async_copy(scale_lines, lines_out, side.at[4]),
    ]
    for copy in last:
        copy.start()
    for copy in stores + last:
        copy.wait()


def place_kernel(
    ranges, entries_in, table_in, arrived, cache, scale_out, entries, places, seen, table, scale, held, load, store, side
):
    sources = arrived.shape[0]
    rows = cache.shape[1]
    step = sources // 16
    loads = []
    for i in range(16):
        part = pl.ds(i * step, step)
        loads.append(pltpu.make_async_copy(arrived.at[part], held.at[part], load.at[i]))
        loads[-1].start()
    small = [
        pltpu.make_async_copy(*pair, side.at[i])
        for i, pair in enumerate(((entries_in, entries), (table_in, table)))
    ]
    for copy in small:
        copy.start()
    for d in range(sources):
        seen[d] = 0
    members, _, span = scale.shape
    slots = table.shape[1] // 2
    first_row = lax.axis_index("grp") * members
    first_column = lax.axis_index("seq") * span
    small[0].wait()
    for b in range(members):
        for j in range(span):
            source = entries[first_row + b, first_column + j] >> (slots.bit_length() - 1)
            count = seen[source] & 1
            seen[source] = count + 1
            places[count, source] = b * span + j
    stores = []
    for d, (s, g) in enumerate(ranked(sources // ranges, ranges)):
        source = s * (sources // ranges) + g
        if d % step == 0:
            loads[d // step].wait()
        for k in range(2):
            stores.append(
                pltpu.make_async_copy(
                    held.at[d, pl.ds(k * rows, rows)], cache.at[places[k, source]], store.at[2 * d + k]
                )
            )
            stores[-1].start()
    small[1].wait()
    row = lax.broadcasted_iota(jnp.int32, (8, 128), 0)
    lane = lax.broadcasted_iota(jnp.int32, (8, 128), 1)
    for b in range(members):
        lines = jnp.zeros((8, 128), jnp.float32)
        for j in range(span):
            entry = entries[first_row + b, first_column + j]
            source, slot = entry >> (slots.bit_length() - 1), entry & (slots - 1)
            pair = jnp.where(row == 0, table[source, slot], table[source, slots + slot])
            lines = jnp.where(lane == j, pair, lines)
        scale[b] = lines[:2, :span].astype(scale.dtype)
    for one in stores[:16]:
        one.wait()
    copy = pltpu.make_async_copy(scale, scale_out, side.at[3])
    copy.start()
    for one in stores[16:]:
        one.wait()
    copy.wait()


def stat_rows(peak, total, scale_line, half):
    row = lax.broadcasted_iota(jnp.int32, (half, 128), 0)
    lane = lax.broadcasted_iota(jnp.int32, (half, 128), 1)
    peak_row = jnp.sum(jnp.where(row == lane, peak, 0.0), axis=0, keepdims=True)
    total_row = jnp.sum(jnp.where(row == lane, total, 0.0), axis=0, keepdims=True)
    line = lax.broadcasted_iota(jnp.int32, (8, 128), 0)
    lines = jnp.where(line == 1, total_row, jnp.where(line == 2, scale_line, 0.0))
    return jnp.where(line == 0, peak_row, lines)


def as_column(line, half):
    row = lax.broadcasted_iota(jnp.int32, (half, 128), 0)
    lane = lax.broadcasted_iota(jnp.int32, (half, 128), 1)
    return jnp.sum(jnp.where(row == lane, line, 0.0), axis=1, keepdims=True)


def attend_kernel(
    sizes, codes, scales, lens, scale_lines, own_q, other_q, blocks, keep, give, held, peaks, totals, sem
):
    groups, ranges, slots, span, root_scale = sizes
    cores = 2
    chips = groups // cores
    bits, span_bits = slots.bit_length() - 1, span.bit_length() - 1
    size = blocks.shape[2]
    heads = own_q.shape[1] // 2
    group = lax.axis_index("grp")
    chip, core = group >> 1, group & 1
    order = [(flip, k) for flip in range(cores) for k in range(chips)]
    copies = []
    for i, (flip, k) in enumerate(order):
        g = cores * (chip ^ k) + (core ^ flip)
        for s in range(ranges):
            n = i * ranges + s
            copy = pltpu.make_async_copy(
                blocks.at[rank_of(s, g, groups, ranges), pl.ds(0, 4 * size)], held.at[n], sem.at[n]
            )
            copy.start()
            copies.append(copy)
    line = lax.broadcasted_iota(jnp.int32, (2 * heads, size), 0)
    lane = lax.broadcasted_iota(jnp.int32, (2 * heads, size), 1)
    parts = []
    for copy in copies:
        copy.wait()
    for i, (flip, k) in enumerate(order):
        at = chip ^ k
        g = cores * at + (core ^ flip)
        query = (other_q if flip else own_q)[k]
        scored, lives, values = [], [], []
        for s in range(ranges):
            for kk in range(2):
                code = code_at(codes, ranges, kk, g, s)
                slot, place = code & (slots - 1), code >> bits
                member, column = place >> span_bits, place & (span - 1)
                limit = lens[2 * g + member] - (s * span + column) * size
                keys = held[i * ranges + s, pl.ds(2 * kk * size, size)]
                score = lax.dot_general(
                    query, keys, (((1,), (1,)), ((), ())), preferred_element_type=jnp.float32
                )
                low = member * heads
                live = (line >= low) & (line < low + heads) & (lane < limit)
                scored.append(
                    jnp.where(live, score * scales[0, slot] * root_scale, absent_score)
                )
                lives.append(live)
                values.append(scales[1, slot])
        peak = functools.reduce(jnp.maximum, scored)
        peak = jnp.max(peak, axis=1, keepdims=True)
        parts.append((at, flip, peak, scored, lives, values))
    for i, (at, flip, peak, scored, lives, values) in enumerate(parts):
        total, summed = 0.0, 0.0
        for n, (score, live, value) in enumerate(zip(scored, lives, values)):
            weight = jnp.where(live, jnp.exp(score - peak), 0.0)
            total = total + weight
            rows = held[i * ranges + n // 2, pl.ds((2 * (n % 2) + 1) * size, size)]
            summed = summed + jnp.dot(
                (weight * value).astype(jnp.bfloat16), rows, preferred_element_type=jnp.float32
            )
        total = jnp.sum(total, axis=1, keepdims=True)
        to = pl.ds(pl.multiple_of(at * 2 * heads, 2 * heads), 2 * heads)
        (give if flip else keep)[to, :] = summed
        peaks[flip, to, :] = jnp.broadcast_to(peak, (2 * heads, 128))
        totals[flip, to, :] = jnp.broadcast_to(total, (2 * heads, 128))
    half = chips * 2 * heads
    for flip, out in enumerate((keep, give)):
        out[pl.ds(half, 8), :] = stat_rows(
            peaks[flip], totals[flip], scale_lines[pl.ds(2, 1), :], half
        )


def in_three(value):
    parts = []
    for _ in range(3):
        part = value.astype(jnp.bfloat16)
        parts.append(part)
        value = value - part.astype(jnp.float32)
    return parts


def stats_of(part, half):
    tile = part[pl.ds(half, part.shape[0] - half), :].astype(jnp.float32)
    if part.dtype == jnp.float32:
        return tile[0:1], tile[1:2], [tile[2:3]]
    return (
        tile[2:3] + tile[1:2] + tile[0:1],
        tile[5:6] + tile[4:5] + tile[3:4],
        [tile[i : i + 1] for i in range(6, 14)],
    )


def merged(half, *parts):
    stats = [stats_of(part, half) for part in parts]
    peak = functools.reduce(jnp.maximum, [own_peak for own_peak, *_ in stats])
    total, summed = 0.0, 0.0
    for part, (own_peak, own_total, _) in zip(parts, stats):
        factor = jnp.exp(own_peak - peak)
        total = total + own_total * factor
        summed = summed + part[pl.ds(0, half), :].astype(jnp.float32) * as_column(factor, half)
    return peak, total, summed, [scales for *_, scales in stats]


def merge_kernel(*refs):
    *parts, out = refs
    half = out.shape[0] - 16
    peak, total, summed, scales = merged(half, *parts)
    out[pl.ds(0, half), :] = summed.astype(out.dtype)
    line = lax.broadcasted_iota(jnp.int32, (16, 128), 0)
    tile = jnp.zeros((16, 128), jnp.float32)
    for i, part in enumerate(in_three(peak) + in_three(total)):
        tile = jnp.where(line == i, part.astype(jnp.float32), tile)
    chip, core = lax.axis_index("grp") >> 1, lax.axis_index("grp") & 1
    for k, lines in enumerate(scales):
        if len(lines) == 1:
            tile = jnp.where(line == 6 + (core ^ k), lines[0], tile)
        else:
            for i in range(2):
                tile = jnp.where(line == 6 + 2 * (chip ^ k) + i, lines[i], tile)
    out[pl.ds(half, 16), :] = tile.astype(out.dtype)


def finish_kernel(*refs):
    *parts, out, table = refs
    half = out.shape[0]
    _, total, summed, scales = merged(half, *parts)
    out[...] = summed / as_column(total, half)
    here = lax.axis_index("seq")
    for k, lines in enumerate(scales):
        to = pl.ds(pl.multiple_of((here ^ k) * len(lines), len(lines)), len(lines))
        table[to, :] = jnp.concatenate(lines, axis=0)


def project_kernel(own, other, weight, keep, give, slots):
    size = own.shape[1]
    heads = weight.shape[0] // size
    lines = own.shape[0] // heads
    summed = 0.0
    for k in range(heads):
        rows = jnp.concatenate(
            [ref[pl.ds(k, lines, stride=heads), :] for ref in (own, other)], axis=0
        )
        summed = summed + jnp.dot(
            rows.astype(jnp.bfloat16),
            weight[pl.ds(k * size, size), :],
            preferred_element_type=jnp.float32,
        )
    core = lax.axis_index("grp") & 1
    here = lax.axis_index("tp")
    count = keep.shape[0]
    for flip in range(2):
        for at in range(lines // 2):
            j = (2 * at + (core ^ flip)) ^ here
            first = flip * lines + 2 * at
            pair = j >> 1
            given = (j & 1) ^ jnp.where(pair == 2, 1, 0)
            slots[pair + count * given] = summed[first : first + 2]
    keep[...] = slots[pl.ds(0, count)]
    give[...] = slots[pl.ds(count, count)]


def split_kernel(keep, came, *outs):
    for i, out in enumerate(outs):
        out[...] = keep[i] + came[i]


def add_kernel(*refs):
    *terms, out = refs
    total = terms[0][...]
    for term in terms[1:]:
        total = total + term[...]
    out[...] = total.astype(out.dtype)


tight = pltpu.CompilerParams(vmem_limit_bytes=4 * 1024 * 1024)
wide = pltpu.CompilerParams(vmem_limit_bytes=60 * 1024 * 1024)
middle = pltpu.CompilerParams(vmem_limit_bytes=50 * 1024 * 1024)
smem = pl.BlockSpec(memory_space=pltpu.SMEM)
vmem = pl.BlockSpec(memory_space=pltpu.VMEM)
hbm = pl.BlockSpec(memory_space=pltpu.HBM)


def flipped(array, y=0, z=0, x=0, core=0):
    tps, grps = lax.axis_size("tp"), lax.axis_size("grp")
    pairs = []
    for i in range(lax.axis_size("seq") * tps * grps):
        a, b, c = i // (tps * grps), i // grps % tps, i % grps
        pairs.append((i, ((a ^ y) * tps + (b ^ z)) * grps + (c ^ (2 * x + core))))
    return lax.ppermute(array, all_axes, pairs)


def merge(parts, kernel, out_shape):
    return pl.pallas_call(
        kernel,
        out_shape=out_shape,
        in_specs=[vmem] * len(parts),
        out_specs=jax.tree.map(lambda _: vmem, out_shape),
        compiler_params=tight,
    )(*parts)


def per_device(queries, cache_pool, block_scale, block_table, lengths, output_weight):
    seq_count = lax.axis_size("seq")
    group_count = lax.axis_size("grp")
    tp_count = lax.axis_size("tp")
    sources = seq_count * group_count
    chips = group_count // 2
    pool_slots = cache_pool.shape[0]
    key_heads = cache_pool.shape[1]
    block_size = cache_pool.shape[3]
    head_size = cache_pool.shape[4]
    batch_rows, table_width = block_table.shape
    per_group = batch_rows // group_count
    share_blocks = table_width // seq_count
    heads_here = queries.shape[1]
    out_width = output_weight.shape[1]
    root_scale = 1.0 / math.sqrt(head_size)
    rows = 2 * block_size

    flat_queries = queries.reshape(per_group * heads_here, head_size)
    abroad = flipped(flat_queries, z=1)
    outgoing, codes, scale_lines = pl.pallas_call(
        functools.partial(gather_kernel, (group_count, seq_count, pool_slots, share_blocks)),
        out_shape=(
            jax.ShapeDtypeStruct((sources, 2 * rows, head_size), cache_pool.dtype),
            jax.ShapeDtypeStruct(block_table.shape, jnp.int32),
            jax.ShapeDtypeStruct((8, 128), jnp.float32),
        ),
        in_specs=[hbm, hbm, hbm],
        out_specs=(hbm, hbm, hbm),
        scratch_shapes=[
            pltpu.VMEM(block_table.shape, jnp.int32),
            pltpu.VMEM((2, pool_slots), block_scale.dtype),
            pltpu.VMEM(block_table.shape, jnp.int32),
            pltpu.VMEM((8, 128), jnp.float32),
            pltpu.VMEM((pool_slots, rows, head_size), cache_pool.dtype),
            pltpu.SMEM(block_table.shape, jnp.int32),
            pltpu.SemaphoreType.DMA((8,)),
            pltpu.SemaphoreType.DMA((2 * sources,)),
            pltpu.SemaphoreType.DMA((5,)),
        ],
        compiler_params=wide,
    )(
        block_table,
        block_scale.reshape(pool_slots, 2).T,
        cache_pool.reshape(pool_slots, rows, head_size),
    )
    outgoing, abroad = lax.optimization_barrier((outgoing, abroad))
    order = [s * group_count + g for s, g in ranked(group_count, seq_count)]
    arrived = lax.all_to_all(
        outgoing, both_axes, split_axis=0, concat_axis=0, axis_index_groups=[order], tiled=True
    )

    own_q = jnp.stack(
        [flat_queries] + [flipped(abroad, x=k, z=1) for k in range(1, chips)]
    )
    other_q = flipped(own_q, core=1)

    half = chips * per_group * heads_here
    line_shape = jax.ShapeDtypeStruct((half + 8, head_size), jnp.float32)
    keep, give = pl.pallas_call(
        functools.partial(
            attend_kernel, (group_count, seq_count, pool_slots, share_blocks, root_scale)
        ),
        out_shape=(line_shape, line_shape),
        in_specs=[smem, smem, smem, vmem, vmem, vmem, hbm],
        out_specs=(vmem, vmem),
        scratch_shapes=[
            pltpu.VMEM((sources, 2 * rows, head_size), cache_pool.dtype),
            pltpu.VMEM((2, half, 128), jnp.float32),
            pltpu.VMEM((2, half, 128), jnp.float32),
            pltpu.SemaphoreType.DMA((sources,)),
        ],
        compiler_params=middle,
    )(codes, scale_lines, lengths, scale_lines, own_q, other_q, outgoing)
    message = jax.ShapeDtypeStruct((half + 16, head_size), jnp.bfloat16)
    lines = merge([keep, flipped(give, core=1)], merge_kernel, message)
    lines = merge([flipped(lines, z=1, x=k) for k in range(chips)], merge_kernel, message)
    lines, scale_table = merge(
        [flipped(lines, z=1, y=k) for k in range(seq_count)],
        finish_kernel,
        (
            jax.ShapeDtypeStruct((half, head_size), jnp.float32),
            jax.ShapeDtypeStruct((sources, 128), jnp.float32),
        ),
    )
    other_lines = flipped(lines, core=1)
    pair_shape = jax.ShapeDtypeStruct((tp_count // 2, per_group, out_width), jnp.float32)
    keep, give = pl.pallas_call(
        project_kernel,
        out_shape=(pair_shape, pair_shape),
        in_specs=[vmem, vmem, vmem],
        out_specs=(vmem, vmem),
        scratch_shapes=[pltpu.VMEM((tp_count, per_group, out_width), jnp.float32)],
        compiler_params=tight,
    )(lines, other_lines, output_weight)
    share = jax.ShapeDtypeStruct((per_group, out_width), jnp.float32)
    shares = pl.pallas_call(
        split_kernel,
        out_shape=(share,) * (tp_count // 2),
        in_specs=[vmem, vmem],
        out_specs=(vmem,) * (tp_count // 2),
        compiler_params=tight,
    )(keep, flipped(give, z=1))
    terms = [shares[0]] + [flipped(shares[i], z=z) for i, z in ((1, 2), (2, 5), (3, 6))]
    placed, scales = pl.pallas_call(
        functools.partial(place_kernel, seq_count),
        out_shape=(
            jax.ShapeDtypeStruct((pool_slots, rows, head_size), cache_pool.dtype),
            jax.ShapeDtypeStruct((per_group, 2, share_blocks), block_scale.dtype),
        ),
        in_specs=[hbm, vmem, hbm],
        out_specs=(hbm, hbm),
        scratch_shapes=[
            pltpu.SMEM(block_table.shape, jnp.int32),
            pltpu.SMEM((2, sources), jnp.int32),
            pltpu.SMEM((sources,), jnp.int32),
            pltpu.SMEM((sources, 128), jnp.float32),
            pltpu.VMEM((per_group, 2, share_blocks), block_scale.dtype),
            pltpu.VMEM((sources, 2 * rows, head_size), cache_pool.dtype),
            pltpu.SemaphoreType.DMA((16,)),
            pltpu.SemaphoreType.DMA((2 * sources,)),
            pltpu.SemaphoreType.DMA((4,)),
        ],
        compiler_params=middle,
    )(block_table, scale_table, arrived)
    terms, scales = lax.optimization_barrier((terms, scales))
    summed = pl.pallas_call(
        add_kernel,
        out_shape=jax.ShapeDtypeStruct((per_group, out_width), jnp.bfloat16),
        in_specs=[vmem] * len(terms),
        out_specs=vmem,
        compiler_params=tight,
    )(*terms)
    decode_cache = placed.reshape(
        per_group, share_blocks, key_heads, 2, block_size, head_size
    )
    decode_scale = scales.transpose(0, 2, 1).reshape(per_group, share_blocks, key_heads, 2)
    return (summed, decode_cache, decode_scale)


def solution(mesh):
    placed = (
        P("grp", "tp", None),
        P(("seq", "grp"), "tp", None, None, None),
        P(("seq", "grp"), "tp", None),
        P(),
        P(),
        P("tp", ("seq", "grp")),
    )
    return jax.shard_map(
        per_device,
        mesh=mesh,
        in_specs=placed,
        out_specs=(
            P("tp", ("seq", "grp")),
            P("grp", "seq", "tp", None, None, None),
            P("grp", "seq", "tp", None),
        ),
        check_vma=False,
    )
```
